32 devices in a mesh: trial: 4 (over x, core), shard: 4 (over z), tp: 2 (over y).
Axes of the slice: x: 2, y: 2, z: 4, core: 2. Of those that a mesh axis runs over, the one named last changes fastest.
Arguments:
- weight_query: bfloat16 [10240, 4096], P(('trial', 'shard'), 'tp'), parts along dimension 0, may hold values from -0.125 to 0.125
- low_query: bfloat16 [10240, 64], P(('trial', 'shard')), parts along dimension 0, may hold values from -0.125 to 0.125
- high_query: bfloat16 [256, 4096], P('trial', 'tp'), parts along dimension 0, may hold values from -0.75 to 0.75
- weight_key: bfloat16 [10240, 1024], P(('trial', 'shard'), 'tp'), parts along dimension 0, may hold values from -0.125 to 0.125
- low_key: bfloat16 [10240, 64], P(('trial', 'shard')), parts along dimension 0, may hold values from -0.125 to 0.125
- high_key: bfloat16 [256, 1024], P('trial', 'tp'), parts along dimension 0, may hold values from -0.75 to 0.75
- weight_value: bfloat16 [10240, 1024], P(('trial', 'shard'), 'tp'), parts along dimension 0, may hold values from -0.125 to 0.125
- low_value: bfloat16 [10240, 64], P(('trial', 'shard')), parts along dimension 0, may hold values from -0.125 to 0.125
- high_value: bfloat16 [256, 1024], P('trial', 'tp'), parts along dimension 0, may hold values from -0.75 to 0.75
- norm_train: float32 [10240], P(('trial', 'shard', 'tp')), parts along dimension 0, may hold values from 0.25 to 1.75
- norm_step: float32 [10240], P(('trial', 'shard', 'tp')), parts along dimension 0, may hold values from -0.3 to 0.3
Outputs:
- serve_query: bfloat16 [16384, 2560], P(('trial', 'tp')), parts along dimension 0
- serve_key: bfloat16 [4096, 2560], P(('trial', 'tp')), parts along dimension 0
- serve_value: bfloat16 [4096, 2560], P(('trial', 'tp')), parts along dimension 0
- serve_norm: bfloat16 [10240], P('trial'), parts along dimension 0
The draws below stay inside these ranges and needn't reach their ends.
There are 4 independent parts, one for each index of `trial`. The reference program is written for one: setup_inputs(seed, part) draws one part's arguments, and reference() takes and returns one part's arrays. A program takes and returns all parts, laid end to end along the dimension named above; each array names one. Nothing has to cross between parts.
All inputs are finite; a program needn't handle non-finite values.
Results may differ from the reference program's by a relative error of at most 0.001.
Values may be sent and summed in bfloat16 or wider, within the bound.
A program may use at most 128 MiB of HBM per device.

```python
import jax
import jax.numpy as jnp

D_MODEL = 2560
Q_DIM = 4096
KV_DIM = 1024
RANK = 64


def levels(stream_key, shape, split, low, top_value):
    factor_of = 1.0
    for dim, parts in split:
        steps = jax.random.uniform(jax.random.fold_in(jax.random.fold_in(stream_key, 6), dim), (parts,), jnp.float32, low / len(split), top_value / len(split))
        factor_of = factor_of * jnp.repeat(jnp.exp(steps), shape[dim] // parts).reshape((-1,) + (1,) * (len(shape) - 1 - dim))
    return factor_of


def normal_values(key, dims, scale, reach, split=(), dtype=jnp.bfloat16):
    level = levels(key, dims, split, -0.22, 0.18) if split else 1.0
    entries = jax.random.normal(key, dims, jnp.float32) * scale * level
    return jnp.minimum(jnp.maximum(entries, -reach), reach).astype(dtype)


def setup_inputs(seed: int = 0, part: int = 0) -> dict:
    keys = jax.random.split(jax.random.key(seed), 12)
    own_keys = jax.random.split(jax.random.fold_in(keys[11], part), 12)
    weight_query = normal_values(own_keys[0], (D_MODEL, Q_DIM), D_MODEL ** -0.5, 0.125, ((0, 4), (1, 2)))
    low_query = normal_values(own_keys[1], (D_MODEL, RANK), D_MODEL ** -0.5, 0.125, ((0, 4),))
    high_query = normal_values(own_keys[2], (RANK, Q_DIM), RANK ** -0.5, 0.75, ((1, 2),))
    weight_key = normal_values(own_keys[3], (D_MODEL, KV_DIM), D_MODEL ** -0.5, 0.125, ((0, 4), (1, 2)))
    low_key = normal_values(own_keys[4], (D_MODEL, RANK), D_MODEL ** -0.5, 0.125, ((0, 4),))
    high_key = normal_values(own_keys[5], (RANK, KV_DIM), RANK ** -0.5, 0.75, ((1, 2),))
    weight_value = normal_values(own_keys[6], (D_MODEL, KV_DIM), D_MODEL ** -0.5, 0.125, ((0, 4), (1, 2)))
    low_value = normal_values(own_keys[7], (D_MODEL, RANK), D_MODEL ** -0.5, 0.125, ((0, 4),))
    high_value = normal_values(own_keys[8], (RANK, KV_DIM), RANK ** -0.5, 0.75, ((1, 2),))
    norm_train = jnp.clip(1.0 + 0.15 * jax.random.normal(own_keys[9], (D_MODEL,), jnp.float32), 0.25, 1.75)
    norm_step = jnp.clip(jax.random.uniform(own_keys[10], (D_MODEL,), jnp.float32, -0.3, 0.3) * levels(own_keys[10], (D_MODEL,), ((0, 8),), -0.4, 0.0), -0.3, 0.3)
    return dict(weight_query=weight_query, low_query=low_query, high_query=high_query, weight_key=weight_key, low_key=low_key, high_key=high_key, weight_value=weight_value, low_value=low_value, high_value=high_value, norm_train=norm_train, norm_step=norm_step)


mix_rate = 1.0


def reference(weight_query, low_query, high_query, weight_key, low_key, high_key, weight_value, low_value, high_value, norm_train, norm_step):
    fresh_query = weight_query.astype(jnp.float32) + mix_rate * jnp.dot(low_query, high_query, preferred_element_type=jnp.float32)
    fresh_key = weight_key.astype(jnp.float32) + mix_rate * jnp.dot(low_key, high_key, preferred_element_type=jnp.float32)
    fresh_value = weight_value.astype(jnp.float32) + mix_rate * jnp.dot(low_value, high_value, preferred_element_type=jnp.float32)
    serve_query = fresh_query.T.astype(jnp.bfloat16)
    serve_key = fresh_key.T.astype(jnp.bfloat16)
    serve_value = fresh_value.T.astype(jnp.bfloat16)
    serve_norm = (norm_train + norm_step).astype(jnp.bfloat16)
    return serve_query, serve_key, serve_value, serve_norm
```

```python
import functools

import jax
import jax.numpy as jnp
from jax import lax
from jax.experimental import pallas as pl
from jax.experimental.pallas import tpu as pltpu
from jax.sharding import PartitionSpec as P

mix_rate = 1.0
MESH = pl.DeviceIdType.MESH
ROWS = 128
LATE = (4, 1)


def late_from(count):
    first = [max(count - late, 0) for late in LATE]
    core = lax.rem(lax.axis_index("trial"), 2)
    return jnp.where(core == 0, first[0], first[1])


def gather_kernel(n, tp, rows, *refs):
    weights, low_refs, high_refs = refs[0:3], refs[3:6], refs[6:9]
    norm_train, norm_step = refs[9:11]
    outs = refs[11:14]
    norm_out = refs[14]
    staged, lows, highs = refs[15], refs[16:19], refs[19:22]
    (norm_all, load_sem, small_sem, send_sem, recv_sem,
     chain_send, chain_recv, side_send, side_recv, norm_flat) = refs[22:]
    me, my_tp = lax.axis_index("shard"), lax.axis_index("tp")
    depth = staged.shape[1]
    counts = [weight.shape[1] // rows for weight in weights]
    starts = [sum(counts[:i]) for i in range(len(counts))]
    total = sum(counts)
    held_back = late_from(counts[-1])
    last = len(counts) - 1

    def load(which, c):
        return pltpu.make_async_copy(
            weights[which].at[:, pl.ds(pl.multiple_of(c * rows, rows), rows)],
            staged.at[starts[which] + c],
            load_sem.at[starts[which] + c],
        )

    small = [
        (
            pltpu.make_async_copy(low_refs[i], lows[i], small_sem.at[2 * i]),
            pltpu.make_async_copy(high_refs[i], highs[i], small_sem.at[2 * i + 1]),
        )
        for i in range(3)
    ]

    barrier = pltpu.get_barrier_semaphore()
    for way in (1, -1):
        @pl.when((me + way >= 0) & (me + way < n))
        def _():
            pl.semaphore_signal(
                barrier, inc=1, device_id={"shard": jnp.clip(me + way, 0, n - 1)},
                device_id_type=MESH,
            )
    for t in range(1, tp):
        pl.semaphore_signal(
            barrier, inc=1, device_id={"tp": lax.rem(my_tp + t, tp)}, device_id_type=MESH
        )
    for which in range(3):
        for copy in small[which]:
            copy.start()

        @pl.loop(0, counts[which])
        def _(c):
            load(which, c).start()

    def block(which, c, owner):
        return outs[which].at[
            pl.ds(pl.multiple_of(c * rows, rows), rows),
            pl.ds(pl.multiple_of(owner * depth, 128), depth),
        ]

    def lane(step, way):
        return (0 if way > 0 else 1) * (n - 1) + step

    def ahead(way):
        return {"shard": jnp.clip(me + way, 0, n - 1)}

    def hop(which, c, step, way, owner):
        here = block(which, c, owner)
        slot = lane(step, way) * total + starts[which] + c
        return pltpu.make_async_remote_copy(
            here, here, send_sem.at[slot], recv_sem.at[slot],
            device_id=ahead(way), device_id_type=MESH,
        )

    def chain(step, way, owner):
        here = norm_all.at[owner * tp + my_tp]
        return pltpu.make_async_remote_copy(
            here, here, chain_send.at[lane(step, way)], chain_recv.at[lane(step, way)],
            device_id=ahead(way), device_id_type=MESH,
        )

    def side(owner, t, tp_of):
        here = norm_all.at[owner * tp + tp_of]
        slot = owner * (tp - 1) + t - 1
        return pltpu.make_async_remote_copy(
            here, here, side_send.at[slot], side_recv.at[slot],
            device_id={"tp": lax.rem(my_tp + t, tp)}, device_id_type=MESH,
        )

    def end(at, way):
        return at == (n - 1 if way > 0 else 0)

    def sends(step, way):
        owner = me - way * step
        ok = (owner >= 0) & (owner < n) & (me + way >= 0) & (me + way < n)
        return ok, jnp.clip(owner, 0, n - 1)

    def arrives(step, way):
        owner = me - way * (step + 1)
        return (owner >= 0) & (owner < n), jnp.clip(owner, 0, n - 1)

    def now(which, c, at, way):
        if which != last:
            return True
        return (c < held_back) | jnp.logical_not(end(at, way))

    def send(which, c, step):
        for way in (1, -1):
            ok, owner = sends(step, way)
            ok = ok & now(which, c, me + way, way)
            pl.when(ok)(lambda: hop(which, c, step, way, owner).start())

    def merge(which, c):
        load(which, c).wait()
        high = highs[which][:, pl.ds(pl.multiple_of(c * rows, rows), rows)]
        fresh = staged[starts[which] + c].astype(jnp.float32) + mix_rate * lax.dot_general(
            lows[which][...], high, (((0,), (0,)), ((), ())),
            preferred_element_type=jnp.float32,
        )
        outs[which][
            pl.ds(pl.multiple_of(c * rows, rows), rows),
            pl.ds(pl.multiple_of(me * depth, 128), depth),
        ] = fresh.astype(jnp.bfloat16).T

    norm_all[me * tp + my_tp, 0, :] = norm_train[...] + norm_step[...]
    for copy in small[0]:
        copy.wait()
    merge(0, 0)

    inner = jnp.where(me > 0, 1, 0) + jnp.where(me < n - 1, 1, 0)
    pl.semaphore_wait(barrier, inner + tp - 1)
    send(0, 0, 0)
    for way in (1, -1):
        ok, owner = sends(0, way)
        pl.when(ok)(lambda: chain(0, way, owner).start())
    for t in range(1, tp):
        side(me, t, my_tp).start()

    for which in range(3):
        if which:
            for copy in small[which]:
                copy.wait()

        @pl.loop(0 if which else 1, counts[which])
        def _(c):
            merge(which, c)
            send(which, c, 0)

    def pass_norm(step):
        for way in (1, -1):
            ok, owner = arrives(step, way)
            further = ok & (me + way >= 0) & (me + way < n)

            @pl.when(ok)
            def _():
                chain(step, way, owner).wait_recv()
                for t in range(1, tp):
                    side(owner, t, my_tp).start()

            if step < n - 2:
                pl.when(further)(lambda: chain(step + 1, way, owner).start())

    def pass_on(which, c, step):
        for way in (1, -1):
            ok, owner = arrives(step, way)
            further = ok & (me + way >= 0) & (me + way < n) & now(which, c, me + way, way)
            ok = ok & now(which, c, me, way)
            pl.when(ok)(lambda: hop(which, c, step, way, owner).wait_recv())
            if step < n - 2:
                pl.when(further)(lambda: hop(which, c, step + 1, way, owner).start())

    for step in range(n - 1):
        pass_norm(step)
        for which in range(3):
            pl.loop(0, counts[which])(functools.partial(pass_on, which, step=step))

    for owner in range(n):
        for t in range(1, tp):
            side(owner, t, lax.rem(my_tp - t + tp, tp)).wait_recv()
    part = norm_all.shape[2]
    for row in range(norm_out.shape[0]):
        pieces, at = [], row * 128
        while at < (row + 1) * 128:
            slot, lo = divmod(at, part)
            size = min(part - lo, (row + 1) * 128 - at)
            pieces.append(norm_all[slot, 0:1, lo : lo + size])
            at += size
        norm_row = jnp.concatenate(pieces, axis=1) if len(pieces) > 1 else pieces[0]
        norm_flat[row : row + 1, :] = norm_row
    norm_out[...] = norm_flat[...].astype(jnp.bfloat16)

    def sent(which, c, step):
        for way in (1, -1):
            ok, owner = sends(step, way)
            ok = ok & now(which, c, me + way, way)
            pl.when(ok)(lambda: hop(which, c, step, way, owner).wait_send())

    for step in range(n - 1):
        for way in (1, -1):
            ok, owner = sends(step, way)
            pl.when(ok)(lambda: chain(step, way, owner).wait_send())
        for which in range(3):
            pl.loop(0, counts[which])(functools.partial(sent, which, step=step))
    for owner in range(n):
        for t in range(1, tp):
            side(owner, t, my_tp).wait_send()


def gathered(n, tp, rows, weights, lows, highs, train, step):
    depth = weights[0].shape[0]
    total = sum(weight.shape[1] // rows for weight in weights)
    group, part = n * tp, train.shape[0]
    vmem, hbm = pl.BlockSpec(memory_space=pltpu.VMEM), pl.BlockSpec(memory_space=pltpu.HBM)
    return pl.pallas_call(
        functools.partial(gather_kernel, n, tp, rows),
        out_shape=[pltpu.VMEM((weight.shape[1], n * depth), jnp.bfloat16) for weight in weights]
        + [pltpu.VMEM((group * part // 128, 128), jnp.bfloat16)],
        in_specs=[hbm] * 9 + [vmem] * 2,
        out_specs=[vmem] * 4,
        scratch_shapes=[
            pltpu.VMEM((total, depth, rows), jnp.bfloat16),
            *[pltpu.VMEM(x.shape, x.dtype) for x in (*lows, *highs)],
            pltpu.VMEM((group, 1, part), jnp.float32),
            pltpu.SemaphoreType.DMA((total,)),
            pltpu.SemaphoreType.DMA((6,)),
            pltpu.SemaphoreType.DMA((2 * (n - 1) * total,)),
            pltpu.SemaphoreType.DMA((2 * (n - 1) * total,)),
            pltpu.SemaphoreType.DMA((2 * (n - 1),)),
            pltpu.SemaphoreType.DMA((2 * (n - 1),)),
            pltpu.SemaphoreType.DMA((max(n * (tp - 1), 1),)),
            pltpu.SemaphoreType.DMA((max(n * (tp - 1), 1),)),
            pltpu.VMEM((group * part // 128, 128), jnp.float32),
        ],
        compiler_params=pltpu.CompilerParams(
            collective_id=0, has_side_effects=True, vmem_limit_bytes=47 * 2**20
        ),
        name="gather",
    )(*weights, *lows, *highs, train, step)


def flush_kernel(count, *refs):
    sources, results = refs[:count], refs[count : 2 * count]
    token, sems = refs[2 * count :]
    copies = [
        pltpu.make_async_copy(source, result, sems.at[i])
        for i, (source, result) in enumerate(zip(sources, results))
    ]
    for copy in copies:
        copy.start()
    token[...] = jnp.zeros_like(token)
    for copy in copies:
        copy.wait()


def flushed(held):
    return pl.pallas_call(
        functools.partial(flush_kernel, len(held)),
        out_shape=[jax.ShapeDtypeStruct(x.shape, x.dtype) for x in held]
        + [pltpu.VMEM((8, 128), jnp.float32)],
        in_specs=[pl.BlockSpec(memory_space=pltpu.VMEM)] * len(held),
        out_specs=[pl.BlockSpec(memory_space=pltpu.HBM)] * len(held)
        + [pl.BlockSpec(memory_space=pltpu.VMEM)],
        scratch_shapes=[pltpu.SemaphoreType.DMA((len(held),))],
        compiler_params=pltpu.CompilerParams(vmem_limit_bytes=2**20),
        name="flush",
    )(*held)


def tail_kernel(n, rows, depth, held, token, tail, send_sem, recv_sem):
    me = lax.axis_index("shard")
    count = held.shape[0] // rows
    first = late_from(count)
    width = (n - 1) * depth
    ends = ((1, n - 1), (-1, 0))

    barrier = pltpu.get_barrier_semaphore()
    for way, at in ends:
        @pl.when(me == at)
        def _():
            pl.semaphore_signal(
                barrier, inc=1, device_id={"shard": at - way}, device_id_type=MESH
            )

    def copy(c, way, at):
        here = (
            pl.ds(pl.multiple_of(c * rows, rows), rows),
            pl.ds(0 if way > 0 else depth, width),
        )
        slot = (0 if way > 0 else count) + c
        return pltpu.make_async_remote_copy(
            held.at[here], tail.at[here], send_sem.at[slot], recv_sem.at[slot],
            device_id={"shard": at}, device_id_type=MESH,
        )

    greeted = sum(jnp.where(me == at - way, 1, 0) for way, at in ends)
    pl.when(greeted > 0)(lambda: pl.semaphore_wait(barrier, greeted))
    for way, at in ends:
        @pl.when(me == at - way)
        def _():
            pl.loop(first, count)(lambda c: copy(c, way, at).start())
    for way, at in ends:
        @pl.when(me == at)
        def _():
            pl.loop(first, count)(lambda c: copy(c, way, at).wait_recv())
    for way, at in ends:
        @pl.when(me == at - way)
        def _():
            pl.loop(first, count)(lambda c: copy(c, way, at).wait_send())


def tailed(n, rows, depth, held, token):
    vmem = pl.BlockSpec(memory_space=pltpu.VMEM)
    count = held.shape[0] // rows
    return pl.pallas_call(
        functools.partial(tail_kernel, n, rows, depth),
        out_shape=pltpu.VMEM(held.shape, held.dtype),
        in_specs=[vmem, vmem],
        out_specs=vmem,
        scratch_shapes=[
            pltpu.SemaphoreType.DMA((2 * count,)),
            pltpu.SemaphoreType.DMA((2 * count,)),
        ],
        compiler_params=pltpu.CompilerParams(
            collective_id=1, has_side_effects=True, vmem_limit_bytes=2**20
        ),
        name="tail",
    )(held, token)


def close_kernel(n, rows, depth, held, tail, result, sems):
    me = lax.axis_index("shard")
    count = held.shape[0] // rows
    first = late_from(count)
    width = (n - 1) * depth
    outer = (me == 0) | (me == n - 1)

    def whole(c):
        here = pl.ds(pl.multiple_of(c * rows, rows), rows)
        return pltpu.make_async_copy(held.at[here, :], result.at[here, :], sems.at[c])

    def cut(c, at):
        here = pl.ds(pl.multiple_of(c * rows, rows), rows)
        mine = (here, pl.ds(at * depth, depth))
        theirs = (here, pl.ds(0 if at else depth, width))
        return (
            pltpu.make_async_copy(held.at[mine], result.at[mine], sems.at[c]),
            pltpu.make_async_copy(tail.at[theirs], result.at[theirs], sems.at[count + c]),
        )

    bound = jnp.where(outer, first, count)
    pl.loop(0, bound)(lambda c: whole(c).start())
    for at in (0, n - 1):
        @pl.when(me == at)
        def _():
            @pl.loop(first, count)
            def _(c):
                for copy in cut(c, at):
                    copy.start()
    pl.loop(0, bound)(lambda c: whole(c).wait())
    for at in (0, n - 1):
        @pl.when(me == at)
        def _():
            @pl.loop(first, count)
            def _(c):
                for copy in cut(c, at):
                    copy.wait()


def closed(n, rows, depth, held, tail):
    vmem = pl.BlockSpec(memory_space=pltpu.VMEM)
    return pl.pallas_call(
        functools.partial(close_kernel, n, rows, depth),
        out_shape=jax.ShapeDtypeStruct(held.shape, held.dtype),
        in_specs=[vmem, vmem],
        out_specs=pl.BlockSpec(memory_space=pltpu.HBM),
        scratch_shapes=[pltpu.SemaphoreType.DMA((2 * held.shape[0] // rows,))],
        compiler_params=pltpu.CompilerParams(vmem_limit_bytes=2**20),
        name="close",
    )(held, tail)


def plain(weights, lows, highs, norm_new):
    serve = []
    for weight, low, high in zip(weights, lows, highs):
        fresh = weight.astype(jnp.float32) + mix_rate * jnp.dot(
            low, high, preferred_element_type=jnp.float32
        )
        serve.append(
            lax.all_gather(fresh.astype(jnp.bfloat16), "shard", axis=0, tiled=True).T
        )
    norm = lax.all_gather(
        norm_new.astype(jnp.bfloat16), ("shard", "tp"), axis=0, tiled=True
    )
    return (*serve, norm)


def on_device(n, tp, wq, lq, hq, wk, lk, hk, wv, lv, hv, norm_train, norm_step):
    weights, lows, highs = (wq, wk, wv), (lq, lk, lv), (hq, hk, hv)
    depth = wq.shape[0]
    if n < 2 or depth % 128 or any(weight.shape[1] % ROWS for weight in weights):
        return plain(weights, lows, highs, norm_train + norm_step)
    query, key, value, norm = gathered(
        n, tp, ROWS, weights, [low.T for low in lows], highs, norm_train, norm_step
    )
    *done, token = flushed([query, key, norm])
    tail = tailed(n, ROWS, depth, value, token)
    value = closed(n, ROWS, depth, value, tail)
    return (done[0], done[1], value, done[2].reshape(-1))


def solution(mesh):
    in_specs = (
        (P(("trial", "shard"), "tp"), P(("trial", "shard"), None), P("trial", "tp")) * 3
        + (P(("trial", "shard", "tp")),) * 2
    )
    out_specs = (P(("trial", "tp"), None),) * 3 + (P("trial"),)
    body = functools.partial(on_device, mesh.shape["shard"], mesh.shape["tp"])
    return jax.shard_map(
        body, mesh=mesh, in_specs=in_specs, out_specs=out_specs, check_vma=False
    )
```

```python
import functools

import jax
import jax.numpy as jnp
from jax import lax
from jax.experimental import pallas as pl
from jax.experimental.pallas import tpu as pltpu
from jax.sharding import PartitionSpec as P

mix_rate = 1.0
MESH = pl.DeviceIdType.MESH
ROWS = 128
PIECE = 1024
LATE = (1, 2)


def cut(width, sizes):
    pieces, at = [], 0
    while at < width:
        size = min(sizes[len(pieces)] if len(pieces) < len(sizes) else PIECE, width - at)
        pieces.append((at, size))
        at += size
    return pieces


def last_pieces(width):
    return cut(width, [width - ROWS, ROWS])


def is_late(index, count):
    core = lax.rem(lax.axis_index("trial"), 2)
    late = [index >= count - x for x in LATE]
    if late[0] == late[1]:
        return late[0]
    return core == (0 if late[0] else 1)


def gather_kernel(n, tp, rows, *refs):
    weights, low_refs, high_refs = refs[0:3], refs[3:6], refs[6:9]
    norm_train, norm_step = refs[9:11]
    outs = refs[11:14]
    norm_out = refs[14]
    staged, lows, highs = refs[15], refs[16:19], refs[19:22]
    (norm_all, load_sem, small_sem, send_sem, recv_sem,
     chain_send, chain_recv, side_send, side_recv, norm_flat) = refs[22:]
    me, my_tp = lax.axis_index("shard"), lax.axis_index("tp")
    depth = staged.shape[1]
    counts = [weight.shape[1] // rows for weight in weights]
    starts = [sum(counts[:i]) for i in range(len(counts))]
    total = sum(counts)
    last = len(counts) - 1
    plan = [cut(weight.shape[1], [rows, PIECE - rows] if i == 0 else []) for i, weight in enumerate(weights)]
    plan[last] = last_pieces(weights[last].shape[1])
    pieces = [(which, i, *piece) for which in range(3) for i, piece in enumerate(plan[which])]

    def load(which, c):
        return pltpu.make_async_copy(
            weights[which].at[:, pl.ds(pl.multiple_of(c * rows, rows), rows)],
            staged.at[starts[which] + c],
            load_sem.at[starts[which] + c],
        )

    small = [
        (
            pltpu.make_async_copy(low_refs[i], lows[i], small_sem.at[2 * i]),
            pltpu.make_async_copy(high_refs[i], highs[i], small_sem.at[2 * i + 1]),
        )
        for i in range(3)
    ]

    for copy in small[0]:
        copy.start()
    load(0, 0).start()

    barrier = pltpu.get_barrier_semaphore()
    for way in (1, -1):
        @pl.when((me + way >= 0) & (me + way < n))
        def _():
            pl.semaphore_signal(
                barrier, inc=1, device_id={"shard": jnp.clip(me + way, 0, n - 1)},
                device_id_type=MESH,
            )
    for t in range(1, tp):
        pl.semaphore_signal(
            barrier, inc=1, device_id={"tp": lax.rem(my_tp + t, tp)}, device_id_type=MESH
        )
    for which in range(3):
        if which:
            for copy in small[which]:
                copy.start()

        @pl.loop(0 if which else 1, counts[which])
        def _(c):
            load(which, c).start()

    def block(p, owner):
        which, _, start, size = pieces[p]
        return outs[which].at[
            pl.ds(start, size), pl.ds(pl.multiple_of(owner * depth, 128), depth)
        ]

    def lane(step, way):
        return (0 if way > 0 else 1) * (n - 1) + step

    def ahead(way):
        return {"shard": jnp.clip(me + way, 0, n - 1)}

    def hop(p, step, way, owner):
        here = block(p, owner)
        slot = lane(step, way) * len(pieces) + p
        return pltpu.make_async_remote_copy(
            here, here, send_sem.at[slot], recv_sem.at[slot],
            device_id=ahead(way), device_id_type=MESH,
        )

    def chain(step, way, owner):
        here = norm_all.at[owner * tp + my_tp]
        return pltpu.make_async_remote_copy(
            here, here, chain_send.at[lane(step, way)], chain_recv.at[lane(step, way)],
            device_id=ahead(way), device_id_type=MESH,
        )

    def side(owner, t, tp_of):
        here = norm_all.at[owner * tp + tp_of]
        slot = owner * (tp - 1) + t - 1
        return pltpu.make_async_remote_copy(
            here, here, side_send.at[slot], side_recv.at[slot],
            device_id={"tp": lax.rem(my_tp + t, tp)}, device_id_type=MESH,
        )

    def end(at, way):
        return at == (n - 1 if way > 0 else 0)

    def sends(step, way):
        owner = me - way * step
        ok = (owner >= 0) & (owner < n) & (me + way >= 0) & (me + way < n)
        return ok, jnp.clip(owner, 0, n - 1)

    def arrives(step, way):
        owner = me - way * (step + 1)
        return (owner >= 0) & (owner < n), jnp.clip(owner, 0, n - 1)

    def now(p, at, way):
        which, i = pieces[p][:2]
        if which != last:
            return True
        return jnp.logical_not(is_late(i, len(plan[last])) & end(at, way))

    def send(p, step):
        for way in (1, -1):
            ok, owner = sends(step, way)
            ok = ok & now(p, me + way, way)
            pl.when(ok)(lambda: hop(p, step, way, owner).start())

    def merge(which, c):
        load(which, c).wait()
        high = highs[which][:, pl.ds(pl.multiple_of(c * rows, rows), rows)]
        fresh = staged[starts[which] + c].T.astype(jnp.float32) + mix_rate * lax.dot_general(
            high, lows[which][...], (((0,), (0,)), ((), ())),
            preferred_element_type=jnp.float32,
        )
        outs[which][
            pl.ds(pl.multiple_of(c * rows, rows), rows),
            pl.ds(pl.multiple_of(me * depth, 128), depth),
        ] = fresh.astype(jnp.bfloat16)

    norm_all[me * tp + my_tp, 0, :] = norm_train[...] + norm_step[...]
    for copy in small[0]:
        copy.wait()
    merge(0, 0)

    inner = jnp.where(me > 0, 1, 0) + jnp.where(me < n - 1, 1, 0)
    pl.semaphore_wait(barrier, inner + tp - 1)
    send(0, 0)
    for way in (1, -1):
        ok, owner = sends(0, way)
        pl.when(ok)(lambda: chain(0, way, owner).start())
    for t in range(1, tp):
        side(me, t, my_tp).start()

    for p, (which, i, start, size) in enumerate(pieces):
        if p == 0:
            continue
        if which and i == 0:
            for copy in small[which]:
                copy.wait()
        pl.loop(start // rows, (start + size) // rows)(functools.partial(merge, which))
        send(p, 0)

    def pass_norm(step):
        for way in (1, -1):
            ok, owner = arrives(step, way)
            further = ok & (me + way >= 0) & (me + way < n)

            @pl.when(ok)
            def _():
                chain(step, way, owner).wait_recv()
                for t in range(1, tp):
                    side(owner, t, my_tp).start()

            if step < n - 2:
                pl.when(further)(lambda: chain(step + 1, way, owner).start())

    def pass_on(p, step):
        for way in (1, -1):
            ok, owner = arrives(step, way)
            further = ok & (me + way >= 0) & (me + way < n) & now(p, me + way, way)
            ok = ok & now(p, me, way)
            pl.when(ok)(lambda: hop(p, step, way, owner).wait_recv())
            if step < n - 2:
                pl.when(further)(lambda: hop(p, step + 1, way, owner).start())

    for step in range(n - 1):
        pass_norm(step)
        for p in range(len(pieces)):
            pass_on(p, step)

    for owner in range(n):
        for t in range(1, tp):
            side(owner, t, lax.rem(my_tp - t + tp, tp)).wait_recv()
    part = norm_all.shape[2]
    for row in range(norm_out.shape[0]):
        parts, at = [], row * 128
        while at < (row + 1) * 128:
            slot, lo = divmod(at, part)
            size = min(part - lo, (row + 1) * 128 - at)
            parts.append(norm_all[slot, 0:1, lo : lo + size])
            at += size
        norm_row = jnp.concatenate(parts, axis=1) if len(parts) > 1 else parts[0]
        norm_flat[row : row + 1, :] = norm_row
    norm_out[...] = norm_flat[...].astype(jnp.bfloat16)

    def sent(p, step):
        for way in (1, -1):
            ok, owner = sends(step, way)
            ok = ok & now(p, me + way, way)
            pl.when(ok)(lambda: hop(p, step, way, owner).wait_send())

    for step in range(n - 1):
        for way in (1, -1):
            ok, owner = sends(step, way)
            pl.when(ok)(lambda: chain(step, way, owner).wait_send())
        for p in range(len(pieces)):
            sent(p, step)
    for owner in range(n):
        for t in range(1, tp):
            side(owner, t, my_tp).wait_send()


def gathered(n, tp, rows, weights, lows, highs, train, step):
    depth = weights[0].shape[0]
    total = sum(weight.shape[1] // rows for weight in weights)
    group, part = n * tp, train.shape[0]
    vmem, hbm = pl.BlockSpec(memory_space=pltpu.VMEM), pl.BlockSpec(memory_space=pltpu.HBM)
    return pl.pallas_call(
        functools.partial(gather_kernel, n, tp, rows),
        out_shape=[pltpu.VMEM((weight.shape[1], n * depth), jnp.bfloat16) for weight in weights]
        + [pltpu.VMEM((group * part // 128, 128), jnp.bfloat16)],
        in_specs=[hbm] * 9 + [vmem] * 2,
        out_specs=[vmem] * 4,
        scratch_shapes=[
            pltpu.VMEM((total, depth, rows), jnp.bfloat16),
            *[pltpu.VMEM(x.shape, x.dtype) for x in (*lows, *highs)],
            pltpu.VMEM((group, 1, part), jnp.float32),
            pltpu.SemaphoreType.DMA((total,)),
            pltpu.SemaphoreType.DMA((6,)),
            pltpu.SemaphoreType.DMA((2 * (n - 1) * total,)),
            pltpu.SemaphoreType.DMA((2 * (n - 1) * total,)),
            pltpu.SemaphoreType.DMA((2 * (n - 1),)),
            pltpu.SemaphoreType.DMA((2 * (n - 1),)),
            pltpu.SemaphoreType.DMA((max(n * (tp - 1), 1),)),
            pltpu.SemaphoreType.DMA((max(n * (tp - 1), 1),)),
            pltpu.VMEM((group * part // 128, 128), jnp.float32),
        ],
        compiler_params=pltpu.CompilerParams(
            collective_id=0, has_side_effects=True, vmem_limit_bytes=47 * 2**20
        ),
        name="gather",
    )(*weights, *lows, *highs, train, step)


def flush_kernel(n, count, *refs):
    sources, held = refs[:count], refs[count]
    results, result = refs[count + 1 : 2 * count + 1], refs[2 * count + 1]
    token, sems, held_sems = refs[2 * count + 2 :]
    me = lax.axis_index("shard")
    depth = held.shape[1] // n
    pieces = last_pieces(held.shape[0])
    outer = (me == 0) | (me == n - 1)

    def each(act):
        for i, (source, to) in enumerate(zip(sources, results)):
            act(pltpu.make_async_copy(source, to, sems.at[i]))
        for i, (start, size) in enumerate(pieces):
            rows = pl.ds(start, size)
            late = outer & is_late(i, len(pieces))

            @pl.when(jnp.logical_not(late))
            def _():
                act(pltpu.make_async_copy(
                    held.at[rows, :], result.at[rows, :], held_sems.at[i]
                ))

            @pl.when(late)
            def _():
                here = (rows, pl.ds(pl.multiple_of(me * depth, 128), depth))
                act(pltpu.make_async_copy(held.at[here], result.at[here], held_sems.at[i]))

    each(lambda copy: copy.start())
    token[...] = jnp.zeros_like(token)
    each(lambda copy: copy.wait())


def flushed(n, done, held):
    vmem, hbm = pl.BlockSpec(memory_space=pltpu.VMEM), pl.BlockSpec(memory_space=pltpu.HBM)
    return pl.pallas_call(
        functools.partial(flush_kernel, n, len(done)),
        out_shape=[jax.ShapeDtypeStruct(x.shape, x.dtype) for x in (*done, held)]
        + [pltpu.VMEM((8, 128), jnp.float32)],
        in_specs=[vmem] * (len(done) + 1),
        out_specs=[hbm] * (len(done) + 1) + [vmem],
        scratch_shapes=[
            pltpu.SemaphoreType.DMA((len(done),)),
            pltpu.SemaphoreType.DMA((len(last_pieces(held.shape[0])),)),
        ],
        compiler_params=pltpu.CompilerParams(vmem_limit_bytes=2**20),
        name="flush",
    )(*done, held)


def tail_kernel(n, depth, held, token, tail, send_sem, recv_sem):
    me = lax.axis_index("shard")
    pieces = last_pieces(held.shape[0])
    ends = ((1, n - 1), (-1, 0))

    barrier = pltpu.get_barrier_semaphore()
    for way, at in ends:
        @pl.when(me == at)
        def _():
            pl.semaphore_signal(
                barrier, inc=1, device_id={"shard": at - way}, device_id_type=MESH
            )

    def each(way, at, away, act):
        for i, (start, size) in enumerate(pieces):
            here = (pl.ds(start, size), pl.ds(0 if way > 0 else depth, (n - 1) * depth))
            slot = (0 if way > 0 else len(pieces)) + i

            @pl.when((me == at - away) & is_late(i, len(pieces)))
            def _():
                act(pltpu.make_async_remote_copy(
                    held.at[here], tail.at[here], send_sem.at[slot], recv_sem.at[slot],
                    device_id={"shard": at}, device_id_type=MESH,
                ))

    greeted = sum(jnp.where(me == at - way, 1, 0) for way, at in ends)
    pl.when(greeted > 0)(lambda: pl.semaphore_wait(barrier, greeted))
    for way, at in ends:
        each(way, at, way, lambda copy: copy.start())
    for way, at in ends:
        each(way, at, 0, lambda copy: copy.wait_recv())
    for way, at in ends:
        each(way, at, way, lambda copy: copy.wait_send())


def tailed(n, depth, held, token):
    vmem = pl.BlockSpec(memory_space=pltpu.VMEM)
    count = len(last_pieces(held.shape[0]))
    return pl.pallas_call(
        functools.partial(tail_kernel, n, depth),
        out_shape=pltpu.VMEM(held.shape, held.dtype),
        in_specs=[vmem, vmem],
        out_specs=vmem,
        scratch_shapes=[
            pltpu.SemaphoreType.DMA((2 * count,)),
            pltpu.SemaphoreType.DMA((2 * count,)),
        ],
        compiler_params=pltpu.CompilerParams(
            collective_id=1, has_side_effects=True, vmem_limit_bytes=2**20
        ),
        name="tail",
    )(held, token)


def close_kernel(n, tail, begun, result, sems):
    me = lax.axis_index("shard")
    pieces = last_pieces(tail.shape[0])
    depth = tail.shape[1] // n

    def each(act):
        for at in (0, n - 1):
            for i, (start, size) in enumerate(pieces):
                here = (pl.ds(start, size), pl.ds(0 if at else depth, (n - 1) * depth))

                @pl.when((me == at) & is_late(i, len(pieces)))
                def _():
                    act(pltpu.make_async_copy(tail.at[here], result.at[here], sems.at[i]))

    each(lambda copy: copy.start())
    each(lambda copy: copy.wait())


def closed(n, tail, begun):
    hbm = pl.BlockSpec(memory_space=pltpu.HBM)
    return pl.pallas_call(
        functools.partial(close_kernel, n),
        out_shape=jax.ShapeDtypeStruct(begun.shape, begun.dtype),
        in_specs=[pl.BlockSpec(memory_space=pltpu.VMEM), hbm],
        out_specs=hbm,
        input_output_aliases={1: 0},
        scratch_shapes=[pltpu.SemaphoreType.DMA((len(last_pieces(tail.shape[0])),))],
        compiler_params=pltpu.CompilerParams(vmem_limit_bytes=2**20),
        name="close",
    )(tail, begun)


def plain(weights, lows, highs, norm_new):
    serve = []
    for weight, low, high in zip(weights, lows, highs):
        fresh = weight.astype(jnp.float32) + mix_rate * jnp.dot(
            low, high, preferred_element_type=jnp.float32
        )
        serve.append(
            lax.all_gather(fresh.astype(jnp.bfloat16), "shard", axis=0, tiled=True).T
        )
    norm = lax.all_gather(
        norm_new.astype(jnp.bfloat16), ("shard", "tp"), axis=0, tiled=True
    )
    return (*serve, norm)


def on_device(n, tp, wq, lq, hq, wk, lk, hk, wv, lv, hv, norm_train, norm_step):
    weights, lows, highs = (wq, wk, wv), (lq, lk, lv), (hq, hk, hv)
    depth = wq.shape[0]
    if n < 2 or depth % 128 or any(weight.shape[1] % ROWS for weight in weights) or wv.shape[1] < 2 * ROWS:
        return plain(weights, lows, highs, norm_train + norm_step)
    query, key, value, norm = gathered(
        n, tp, ROWS, weights, [low.T for low in lows], highs, norm_train, norm_step
    )
    *done, begun, token = flushed(n, [query, key, norm], value)
    tail = tailed(n, depth, value, token)
    return (done[0], done[1], closed(n, tail, begun), done[2].reshape(-1))


def solution(mesh):
    in_specs = (
        (P(("trial", "shard"), "tp"), P(("trial", "shard"), None), P("trial", "tp")) * 3
        + (P(("trial", "shard", "tp")),) * 2
    )
    out_specs = (P(("trial", "tp"), None),) * 3 + (P("trial"),)
    body = functools.partial(on_device, mesh.shape["shard"], mesh.shape["tp"])
    return jax.shard_map(
        body, mesh=mesh, in_specs=in_specs, out_specs=out_specs, check_vma=False
    )
```

```python
import functools
import math

import jax
import jax.numpy as jnp
from jax import lax
from jax.experimental import pallas as pl
from jax.experimental.pallas import tpu as pltpu
from jax.sharding import PartitionSpec as P

mix_rate = 1.0
MESH = pl.DeviceIdType.MESH
ROWS = 128
PIECE = 1024
LATE = (1, 2)


def cut(width, sizes):
    pieces, at = [], 0
    while at < width:
        size = min(sizes[len(pieces)] if len(pieces) < len(sizes) else PIECE, width - at)
        pieces.append((at, size))
        at += size
    return pieces


def last_pieces(width):
    return cut(width, [width - ROWS, ROWS])


def is_late(index, count):
    core = lax.rem(lax.axis_index("trial"), 2)
    late = [index >= count - x for x in LATE]
    if late[0] == late[1]:
        return late[0]
    return core == (0 if late[0] else 1)


def gather_kernel(n, rows, *refs):
    weights, low_refs, high_refs = refs[0:3], refs[3:6], refs[6:9]
    norms = refs[9:11]
    outs, line = refs[11:14], refs[14]
    staged, lows, highs = refs[15], refs[16:19], refs[19:22]
    (load_sem, small_sem, send_sem, recv_sem, ready,
     train, change, norm_sem, chain_send, chain_recv) = refs[22:]
    me = lax.axis_index("shard")
    depth = staged.shape[1]
    counts = [weight.shape[1] // rows for weight in weights]
    starts = [sum(counts[:i]) for i in range(len(counts))]
    total = sum(counts)
    last = len(counts) - 1
    plan = [cut(weight.shape[1], [rows, 3 * rows] if i == 0 else []) for i, weight in enumerate(weights)]
    plan[last] = last_pieces(weights[last].shape[1])
    pieces = [(which, i, *piece) for which in range(3) for i, piece in enumerate(plan[which])]

    def load(which, c):
        return pltpu.make_async_copy(
            weights[which].at[:, pl.ds(pl.multiple_of(c * rows, rows), rows)],
            staged.at[starts[which] + c],
            load_sem.at[starts[which] + c],
        )

    def low_copy(which):
        return pltpu.make_async_copy(low_refs[which], lows[which], small_sem.at[6 + which])

    def high_part(which, part):
        lo, hi = (0, rows) if part == 0 else (rows, highs[which].shape[1])
        here = (slice(None), pl.ds(lo, hi - lo))
        return pltpu.make_async_copy(
            high_refs[which].at[here], highs[which].at[here], small_sem.at[2 * which + part]
        )

    load(0, 0).start()
    low_copy(0).start()
    high_part(0, 0).start()

    barrier = pltpu.get_barrier_semaphore()

    @pl.when(me < n - 1)
    def _():
        pl.semaphore_signal(
            barrier, inc=1, device_id={"shard": jnp.minimum(me + 1, n - 1)},
            device_id_type=MESH,
        )

    @pl.when(me > 0)
    def _():
        pl.semaphore_wait(barrier, 1)
        pl.semaphore_signal(
            ready, inc=1, device_id={"shard": jnp.maximum(me - 1, 0)}, device_id_type=MESH
        )

    norm_loads = [
        pltpu.make_async_copy(norms[0], train, norm_sem.at[0]),
        pltpu.make_async_copy(norms[1], change, norm_sem.at[1]),
    ]

    def load_rest():
        for copy in norm_loads:
            copy.start()
        for which in range(3):
            if which:
                low_copy(which).start()
                high_part(which, 0).start()
            high_part(which, 1).start()

            @pl.loop(0 if which else 1, counts[which])
            def _(c):
                load(which, c).start()


    def block(p, owner):
        which, _, start, size = pieces[p]
        return outs[which].at[
            pl.ds(start, size), pl.ds(pl.multiple_of(owner * depth, 128), depth)
        ]

    def lane(step, way):
        return (0 if way > 0 else 1) * (n - 1) + step

    def ahead(way):
        return {"shard": jnp.clip(me + way, 0, n - 1)}

    def hop(p, step, way, owner):
        here = block(p, owner)
        slot = lane(step, way) * len(pieces) + p
        return pltpu.make_async_remote_copy(
            here, here, send_sem.at[slot], recv_sem.at[slot],
            device_id=ahead(way), device_id_type=MESH,
        )

    def chain(hops, way, owner):
        here = line.at[owner]
        return pltpu.make_async_remote_copy(
            here, here, chain_send.at[lane(hops, way)], chain_recv.at[lane(hops, way)],
            device_id=ahead(way), device_id_type=MESH,
        )

    def end(at, way):
        return at == (n - 1 if way > 0 else 0)

    def sends(step, way):
        owner = me - way * step
        ok = (owner >= 0) & (owner < n) & (me + way >= 0) & (me + way < n)
        return ok, jnp.clip(owner, 0, n - 1)

    def arrives(step, way):
        owner = me - way * (step + 1)
        return (owner >= 0) & (owner < n), jnp.clip(owner, 0, n - 1)

    def now(p, at, way):
        which, i = pieces[p][:2]
        if which != last:
            return True
        return jnp.logical_not(is_late(i, len(plan[last])) & end(at, way))

    def send(p, way):
        ok, owner = sends(0, way)
        ok = ok & now(p, me + way, way)
        pl.when(ok)(lambda: hop(p, 0, way, owner).start())

    def merge(which, c):
        load(which, c).wait()
        high = highs[which][:, pl.ds(pl.multiple_of(c * rows, rows), rows)]
        fresh = staged[starts[which] + c].T.astype(jnp.float32) + mix_rate * lax.dot_general(
            high, lows[which][...], (((0,), (0,)), ((), ())),
            preferred_element_type=jnp.float32,
        )
        outs[which][
            pl.ds(pl.multiple_of(c * rows, rows), rows),
            pl.ds(pl.multiple_of(me * depth, 128), depth),
        ] = fresh.astype(jnp.bfloat16)

    low_copy(0).wait()
    high_part(0, 0).wait()
    merge(0, 0)

    send(0, -1)
    pl.when(me < n - 1)(lambda: pl.semaphore_wait(ready, 1))
    send(0, 1)
    load_rest()
    for copy in norm_loads:
        copy.wait()
    line[me, 0, :] = train[...] + change[...]
    for way in (1, -1):
        ok, owner = sends(0, way)
        pl.when(ok)(lambda: chain(0, way, owner).start())
    for p, (which, i, start, size) in enumerate(pieces):
        if p == 0:
            continue
        if i == 0:
            low_copy(which).wait()
            high_part(which, 0).wait()
        if i == 0 or p == 1:
            high_part(which, 1).wait()
        pl.loop(start // rows, (start + size) // rows)(functools.partial(merge, which))
        send(p, -1)
        send(p, 1)

    def pass_norm(step):
        for way in (1, -1):
            ok, owner = arrives(step, way)
            further = ok & (me + way >= 0) & (me + way < n)
            pl.when(ok)(lambda: chain(step, way, owner).wait_recv())
            if step < n - 2:
                pl.when(further)(lambda: chain(step + 1, way, owner).start())

    def pass_on(p, step):
        for way in (1, -1):
            ok, owner = arrives(step, way)
            further = ok & (me + way >= 0) & (me + way < n) & now(p, me + way, way)
            ok = ok & now(p, me, way)
            pl.when(ok)(lambda: hop(p, step, way, owner).wait_recv())
            if step < n - 2:
                pl.when(further)(lambda: hop(p, step + 1, way, owner).start())

    for step in range(n - 1):
        pass_norm(step)
        for p in range(len(pieces)):
            pass_on(p, step)

    def sent(p, step):
        for way in (1, -1):
            ok, owner = sends(step, way)
            ok = ok & now(p, me + way, way)
            pl.when(ok)(lambda: hop(p, step, way, owner).wait_send())

    for step in range(n - 1):
        for way in (1, -1):
            ok, owner = sends(step, way)
            pl.when(ok)(lambda: chain(step, way, owner).wait_send())
        for p in range(len(pieces)):
            sent(p, step)


def gathered(n, rows, weights, lows, highs, train, step):
    depth = weights[0].shape[0]
    total = sum(weight.shape[1] // rows for weight in weights)
    vmem, hbm = pl.BlockSpec(memory_space=pltpu.VMEM), pl.BlockSpec(memory_space=pltpu.HBM)
    return pl.pallas_call(
        functools.partial(gather_kernel, n, rows),
        out_shape=[pltpu.VMEM((weight.shape[1], n * depth), jnp.bfloat16) for weight in weights]
        + [pltpu.VMEM((n, 1, train.shape[0]), jnp.float32)],
        in_specs=[hbm] * 11,
        out_specs=[vmem] * 4,
        scratch_shapes=[
            pltpu.VMEM((total, depth, rows), jnp.bfloat16),
            *[pltpu.VMEM(x.shape, x.dtype) for x in (*lows, *highs)],
            pltpu.SemaphoreType.DMA((total,)),
            pltpu.SemaphoreType.DMA((9,)),
            pltpu.SemaphoreType.DMA((2 * (n - 1) * total,)),
            pltpu.SemaphoreType.DMA((2 * (n - 1) * total,)),
            pltpu.SemaphoreType.REGULAR,
            pltpu.VMEM(train.shape, jnp.float32),
            pltpu.VMEM(step.shape, jnp.float32),
            pltpu.SemaphoreType.DMA((2,)),
            pltpu.SemaphoreType.DMA((2 * (n - 1),)),
            pltpu.SemaphoreType.DMA((2 * (n - 1),)),
        ],
        compiler_params=pltpu.CompilerParams(
            collective_id=0, has_side_effects=True, vmem_limit_bytes=47 * 2**20
        ),
        name="gather",
    )(*weights, *lows, *highs, train, step)


def flush_kernel(n, count, *refs):
    sources, held = refs[:count], refs[count]
    results, result = refs[count + 1 : 2 * count + 1], refs[2 * count + 1]
    token, sems, held_sems = refs[2 * count + 2 :]
    me = lax.axis_index("shard")
    depth = held.shape[1] // n
    pieces = last_pieces(held.shape[0])
    outer = (me == 0) | (me == n - 1)

    def each(act):
        for i, (source, to) in enumerate(zip(sources, results)):
            act(pltpu.make_async_copy(source, to, sems.at[i]))
        for i, (start, size) in enumerate(pieces):
            rows = pl.ds(start, size)
            late = outer & is_late(i, len(pieces))

            @pl.when(jnp.logical_not(late))
            def _():
                act(pltpu.make_async_copy(
                    held.at[rows, :], result.at[rows, :], held_sems.at[i]
                ))

            @pl.when(late)
            def _():
                here = (rows, pl.ds(pl.multiple_of(me * depth, 128), depth))
                act(pltpu.make_async_copy(held.at[here], result.at[here], held_sems.at[i]))

    each(lambda copy: copy.start())
    token[...] = jnp.zeros_like(token)
    each(lambda copy: copy.wait())


def flushed(n, done, held):
    vmem, hbm = pl.BlockSpec(memory_space=pltpu.VMEM), pl.BlockSpec(memory_space=pltpu.HBM)
    return pl.pallas_call(
        functools.partial(flush_kernel, n, len(done)),
        out_shape=[jax.ShapeDtypeStruct(x.shape, x.dtype) for x in (*done, held)]
        + [pltpu.VMEM((8, 128), jnp.float32)],
        in_specs=[vmem] * (len(done) + 1),
        out_specs=[hbm] * (len(done) + 1) + [vmem],
        scratch_shapes=[
            pltpu.SemaphoreType.DMA((len(done),)),
            pltpu.SemaphoreType.DMA((len(last_pieces(held.shape[0])),)),
        ],
        compiler_params=pltpu.CompilerParams(vmem_limit_bytes=2**20),
        name="flush",
    )(*done, held)


def lay_out(parts, flat):
    tp, n, _, part = parts.shape
    for row in range(flat.shape[0]):
        cells, at = [], row * 128
        while at < (row + 1) * 128:
            slot, lo = divmod(at, part)
            size = min(part - lo, (row + 1) * 128 - at)
            cells.append(parts[slot % tp, slot // tp, 0:1, lo : lo + size])
            at += size
        flat[row : row + 1, :] = jnp.concatenate(cells, axis=1) if len(cells) > 1 else cells[0]


def tail_kernel(n, tp, depth, held, line, token, tail, norm_out, *scratch):
    lines, norm_flat, send_sem, recv_sem, side_send, side_recv = scratch
    me, my_tp = lax.axis_index("shard"), lax.axis_index("tp")
    pieces = last_pieces(held.shape[0])
    ends = ((1, n - 1), (-1, 0))

    barrier = pltpu.get_barrier_semaphore()
    for way, at in ends:
        @pl.when(me == at)
        def _():
            pl.semaphore_signal(
                barrier, inc=1, device_id={"shard": at - way}, device_id_type=MESH
            )
    for t in range(1, tp):
        pl.semaphore_signal(
            barrier, inc=1, device_id={"tp": lax.rem(my_tp + t, tp)}, device_id_type=MESH
        )
    lines[my_tp] = line[...]
    greeted = sum(jnp.where(me == at - way, 1, 0) for way, at in ends) + tp - 1
    pl.when(greeted > 0)(lambda: pl.semaphore_wait(barrier, greeted))

    def each(way, at, away, act):
        for i, (start, size) in enumerate(pieces):
            here = (pl.ds(start, size), pl.ds(0 if way > 0 else depth, (n - 1) * depth))
            slot = (0 if way > 0 else len(pieces)) + i

            @pl.when((me == at - away) & is_late(i, len(pieces)))
            def _():
                act(pltpu.make_async_remote_copy(
                    held.at[here], tail.at[here], send_sem.at[slot], recv_sem.at[slot],
                    device_id={"shard": at}, device_id_type=MESH,
                ))

    def side(t, column):
        return pltpu.make_async_remote_copy(
            line, lines.at[column], side_send.at[t - 1], side_recv.at[t - 1],
            device_id={"tp": lax.rem(my_tp + t, tp)}, device_id_type=MESH,
        )

    for way, at in ends:
        each(way, at, way, lambda copy: copy.start())
    for t in range(1, tp):
        side(t, my_tp).start()
    for t in range(1, tp):
        side(t, lax.rem(my_tp - t + tp, tp)).wait_recv()
    lay_out(lines, norm_flat)
    norm_out[...] = norm_flat[...].astype(jnp.bfloat16)
    for way, at in ends:
        each(way, at, 0, lambda copy: copy.wait_recv())
    for way, at in ends:
        each(way, at, way, lambda copy: copy.wait_send())
    for t in range(1, tp):
        side(t, my_tp).wait_send()


def tailed(n, tp, depth, held, line, token):
    vmem = pl.BlockSpec(memory_space=pltpu.VMEM)
    count = len(last_pieces(held.shape[0]))
    lines = (tp, *line.shape)
    flat = (math.prod(lines) // 128, 128)
    return pl.pallas_call(
        functools.partial(tail_kernel, n, tp, depth),
        out_shape=[pltpu.VMEM(held.shape, held.dtype), pltpu.VMEM(flat, jnp.bfloat16)],
        in_specs=[vmem] * 3,
        out_specs=[vmem] * 2,
        scratch_shapes=[
            pltpu.VMEM(lines, jnp.float32),
            pltpu.VMEM(flat, jnp.float32),
            pltpu.SemaphoreType.DMA((2 * count,)),
            pltpu.SemaphoreType.DMA((2 * count,)),
            pltpu.SemaphoreType.DMA((max(tp - 1, 1),)),
            pltpu.SemaphoreType.DMA((max(tp - 1, 1),)),
        ],
        compiler_params=pltpu.CompilerParams(
            collective_id=1, has_side_effects=True, vmem_limit_bytes=2**20
        ),
        name="tail",
    )(held, line, token)


def close_kernel(n, tail, norm, begun, result, norm_out, sems):
    me = lax.axis_index("shard")
    pieces = last_pieces(tail.shape[0])
    depth = tail.shape[1] // n

    def each(act):
        for at in (0, n - 1):
            for i, (start, size) in enumerate(pieces):
                here = (pl.ds(start, size), pl.ds(0 if at else depth, (n - 1) * depth))

                @pl.when((me == at) & is_late(i, len(pieces)))
                def _():
                    act(pltpu.make_async_copy(tail.at[here], result.at[here], sems.at[i]))
        act(pltpu.make_async_copy(norm, norm_out, sems.at[len(pieces)]))

    each(lambda copy: copy.start())
    each(lambda copy: copy.wait())


def closed(n, tail, norm, begun):
    vmem, hbm = pl.BlockSpec(memory_space=pltpu.VMEM), pl.BlockSpec(memory_space=pltpu.HBM)
    return pl.pallas_call(
        functools.partial(close_kernel, n),
        out_shape=[jax.ShapeDtypeStruct(x.shape, x.dtype) for x in (begun, norm)],
        in_specs=[vmem, vmem, hbm],
        out_specs=[hbm] * 2,
        input_output_aliases={2: 0},
        scratch_shapes=[pltpu.SemaphoreType.DMA((len(last_pieces(tail.shape[0])) + 1,))],
        compiler_params=pltpu.CompilerParams(vmem_limit_bytes=2**20),
        name="close",
    )(tail, norm, begun)


def plain(weights, lows, highs, norm_new):
    serve = []
    for weight, low, high in zip(weights, lows, highs):
        fresh = weight.astype(jnp.float32) + mix_rate * jnp.dot(
            low, high, preferred_element_type=jnp.float32
        )
        serve.append(
            lax.all_gather(fresh.astype(jnp.bfloat16), "shard", axis=0, tiled=True).T
        )
    norm = lax.all_gather(
        norm_new.astype(jnp.bfloat16), ("shard", "tp"), axis=0, tiled=True
    )
    return (*serve, norm)


def on_device(n, tp, wq, lq, hq, wk, lk, hk, wv, lv, hv, norm_train, norm_step):
    weights, lows, highs = (wq, wk, wv), (lq, lk, lv), (hq, hk, hv)
    depth = wq.shape[0]
    if n < 2 or depth % 128 or any(weight.shape[1] % ROWS for weight in weights) or wv.shape[1] < 2 * ROWS:
        return plain(weights, lows, highs, norm_train + norm_step)
    query, key, value, line = gathered(
        n, ROWS, weights, [low.T for low in lows], highs, norm_train, norm_step
    )
    query, key, begun, token = flushed(n, [query, key], value)
    tail, norm = tailed(n, tp, depth, value, line, token)
    value, norm = closed(n, tail, norm, begun)
    return (query, key, value, norm.reshape(-1))


def solution(mesh):
    in_specs = (
        (P(("trial", "shard"), "tp"), P(("trial", "shard"), None), P("trial", "tp")) * 3
        + (P(("trial", "shard", "tp")),) * 2
    )
    out_specs = (P(("trial", "tp"), None),) * 3 + (P("trial"),)
    body = functools.partial(on_device, mesh.shape["shard"], mesh.shape["tp"])
    return jax.shard_map(
        body, mesh=mesh, in_specs=in_specs, out_specs=out_specs, check_vma=False
    )
```

```python
import functools
import math

import jax
import jax.numpy as jnp
from jax import lax
from jax.experimental import pallas as pl
from jax.experimental.pallas import tpu as pltpu
from jax.sharding import PartitionSpec as P

mix_rate = 1.0
MESH = pl.DeviceIdType.MESH
ROWS = 128
PIECE = 1024
LATE = (2, 1)
YIELD_NS = 4000


def cut(width, sizes):
    pieces, at = [], 0
    while at < width:
        size = min(sizes[len(pieces)] if len(pieces) < len(sizes) else PIECE, width - at)
        pieces.append((at, size))
        at += size
    return pieces


def last_pieces(width):
    return cut(width, [width - ROWS, ROWS])


def is_late(index, count):
    core = lax.rem(lax.axis_index("trial"), 2)
    late = [index >= count - x for x in LATE]
    if late[0] == late[1]:
        return late[0]
    return core == (0 if late[0] else 1)


def gather_kernel(n, rows, *refs):
    weights, low_refs, high_refs = refs[0:3], refs[3:6], refs[6:9]
    norms = refs[9:11]
    outs, line = refs[11:14], refs[14]
    staged, lows, highs = refs[15], refs[16:19], refs[19:22]
    (load_sem, small_sem, send_sem, recv_sem, ready,
     train, change, norm_sem, chain_send, chain_recv) = refs[22:]
    me = lax.axis_index("shard")
    depth = staged.shape[1]
    counts = [weight.shape[1] // rows for weight in weights]
    starts = [sum(counts[:i]) for i in range(len(counts))]
    total = sum(counts)
    last = len(counts) - 1
    plan = [cut(weight.shape[1], [rows, 3 * rows] if i == 0 else []) for i, weight in enumerate(weights)]
    plan[last] = last_pieces(weights[last].shape[1])
    pieces = [(which, i, *piece) for which in range(3) for i, piece in enumerate(plan[which])]

    def load(which, c):
        return pltpu.make_async_copy(
            weights[which].at[:, pl.ds(pl.multiple_of(c * rows, rows), rows)],
            staged.at[starts[which] + c],
            load_sem.at[starts[which] + c],
        )

    def low_copy(which):
        return pltpu.make_async_copy(low_refs[which], lows[which], small_sem.at[6 + which])

    def high_part(which, part):
        lo, hi = (0, rows) if part == 0 else (rows, highs[which].shape[1])
        here = (slice(None), pl.ds(lo, hi - lo))
        return pltpu.make_async_copy(
            high_refs[which].at[here], highs[which].at[here], small_sem.at[2 * which + part]
        )

    load(0, 0).start()
    low_copy(0).start()
    high_part(0, 0).start()

    barrier = pltpu.get_barrier_semaphore()

    @pl.when(me < n - 1)
    def _():
        pl.semaphore_signal(
            barrier, inc=1, device_id={"shard": jnp.minimum(me + 1, n - 1)},
            device_id_type=MESH,
        )

    @pl.when(me > 0)
    def _():
        pl.semaphore_wait(barrier, 1)
        pl.semaphore_signal(
            ready, inc=1, device_id={"shard": jnp.maximum(me - 1, 0)}, device_id_type=MESH
        )

    norm_loads = [
        pltpu.make_async_copy(norms[0], train, norm_sem.at[0]),
        pltpu.make_async_copy(norms[1], change, norm_sem.at[1]),
    ]

    def load_rest():
        for copy in norm_loads:
            copy.start()
        for which in range(3):
            if which:
                low_copy(which).start()
                high_part(which, 0).start()
            high_part(which, 1).start()

            @pl.loop(0 if which else 1, counts[which])
            def _(c):
                load(which, c).start()


    def block(p, owner):
        which, _, start, size = pieces[p]
        return outs[which].at[
            pl.ds(start, size), pl.ds(pl.multiple_of(owner * depth, 128), depth)
        ]

    def lane(step, way):
        return (0 if way > 0 else 1) * (n - 1) + step

    def ahead(way):
        return {"shard": jnp.clip(me + way, 0, n - 1)}

    def hop(p, step, way, owner):
        here = block(p, owner)
        slot = lane(step, way) * len(pieces) + p
        return pltpu.make_async_remote_copy(
            here, here, send_sem.at[slot], recv_sem.at[slot],
            device_id=ahead(way), device_id_type=MESH,
        )

    def chain(hops, way, owner):
        here = line.at[owner]
        return pltpu.make_async_remote_copy(
            here, here, chain_send.at[lane(hops, way)], chain_recv.at[lane(hops, way)],
            device_id=ahead(way), device_id_type=MESH,
        )

    def end(at, way):
        return at == (n - 1 if way > 0 else 0)

    def sends(step, way):
        owner = me - way * step
        ok = (owner >= 0) & (owner < n) & (me + way >= 0) & (me + way < n)
        return ok, jnp.clip(owner, 0, n - 1)

    def arrives(step, way):
        owner = me - way * (step + 1)
        return (owner >= 0) & (owner < n), jnp.clip(owner, 0, n - 1)

    def now(p, at, way):
        which, i = pieces[p][:2]
        if which != last:
            return True
        return jnp.logical_not(is_late(i, len(plan[last])) & end(at, way))

    def send(p, way):
        ok, owner = sends(0, way)
        ok = ok & now(p, me + way, way)
        pl.when(ok)(lambda: hop(p, 0, way, owner).start())

    def merge(which, c):
        load(which, c).wait()
        high = highs[which][:, pl.ds(pl.multiple_of(c * rows, rows), rows)]
        fresh = staged[starts[which] + c].T.astype(jnp.float32) + mix_rate * lax.dot_general(
            high, lows[which][...], (((0,), (0,)), ((), ())),
            preferred_element_type=jnp.float32,
        )
        outs[which][
            pl.ds(pl.multiple_of(c * rows, rows), rows),
            pl.ds(pl.multiple_of(me * depth, 128), depth),
        ] = fresh.astype(jnp.bfloat16)

    low_copy(0).wait()
    high_part(0, 0).wait()
    merge(0, 0)

    send(0, -1)
    pl.when(me < n - 1)(lambda: pl.semaphore_wait(ready, 1))
    send(0, 1)
    load_rest()
    for copy in norm_loads:
        copy.wait()
    line[me, 0, :] = train[...] + change[...]
    for way in (1, -1):
        ok, owner = sends(0, way)
        pl.when(ok)(lambda: chain(0, way, owner).start())
    for p, (which, i, start, size) in enumerate(pieces):
        if p == 0:
            continue
        if i == 0:
            low_copy(which).wait()
            high_part(which, 0).wait()
        if i == 0 or p == 1:
            high_part(which, 1).wait()
        pl.loop(start // rows, (start + size) // rows)(functools.partial(merge, which))
        send(p, -1)
        send(p, 1)

    def pass_norm(step):
        for way in (1, -1):
            ok, owner = arrives(step, way)
            further = ok & (me + way >= 0) & (me + way < n)
            pl.when(ok)(lambda: chain(step, way, owner).wait_recv())
            if step < n - 2:
                pl.when(further)(lambda: chain(step + 1, way, owner).start())

    def pass_on(p, step):
        for way in (1, -1):
            ok, owner = arrives(step, way)
            further = ok & (me + way >= 0) & (me + way < n) & now(p, me + way, way)
            ok = ok & now(p, me, way)
            pl.when(ok)(lambda: hop(p, step, way, owner).wait_recv())
            if step < n - 2:
                pl.when(further)(lambda: hop(p, step + 1, way, owner).start())

    for step in range(n - 1):
        pass_norm(step)
        for p in range(len(pieces)):
            pass_on(p, step)

    def sent(p, step):
        for way in (1, -1):
            ok, owner = sends(step, way)
            ok = ok & now(p, me + way, way)
            pl.when(ok)(lambda: hop(p, step, way, owner).wait_send())

    for step in range(n - 1):
        for way in (1, -1):
            ok, owner = sends(step, way)
            pl.when(ok)(lambda: chain(step, way, owner).wait_send())
        for p in range(len(pieces)):
            sent(p, step)


def gathered(n, rows, weights, lows, highs, train, step):
    depth = weights[0].shape[0]
    total = sum(weight.shape[1] // rows for weight in weights)
    vmem, hbm = pl.BlockSpec(memory_space=pltpu.VMEM), pl.BlockSpec(memory_space=pltpu.HBM)
    return pl.pallas_call(
        functools.partial(gather_kernel, n, rows),
        out_shape=[pltpu.VMEM((weight.shape[1], n * depth), jnp.bfloat16) for weight in weights]
        + [pltpu.VMEM((n, 1, train.shape[0]), jnp.float32)],
        in_specs=[hbm] * 11,
        out_specs=[vmem] * 4,
        scratch_shapes=[
            pltpu.VMEM((total, depth, rows), jnp.bfloat16),
            *[pltpu.VMEM(x.shape, x.dtype) for x in (*lows, *highs)],
            pltpu.SemaphoreType.DMA((total,)),
            pltpu.SemaphoreType.DMA((9,)),
            pltpu.SemaphoreType.DMA((2 * (n - 1) * total,)),
            pltpu.SemaphoreType.DMA((2 * (n - 1) * total,)),
            pltpu.SemaphoreType.REGULAR,
            pltpu.VMEM(train.shape, jnp.float32),
            pltpu.VMEM(step.shape, jnp.float32),
            pltpu.SemaphoreType.DMA((2,)),
            pltpu.SemaphoreType.DMA((2 * (n - 1),)),
            pltpu.SemaphoreType.DMA((2 * (n - 1),)),
        ],
        compiler_params=pltpu.CompilerParams(
            collective_id=0, has_side_effects=True, vmem_limit_bytes=47 * 2**20
        ),
        name="gather",
    )(*weights, *lows, *highs, train, step)


def flush_kernel(n, count, *refs):
    sources, held = refs[:count], refs[count]
    results, result = refs[count + 1 : 2 * count + 1], refs[2 * count + 1]
    token, sems, held_sems = refs[2 * count + 2 :]
    me = lax.axis_index("shard")
    depth = held.shape[1] // n
    pieces = last_pieces(held.shape[0])
    outer = (me == 0) | (me == n - 1)

    def each(act):
        for i, (source, to) in enumerate(zip(sources, results)):
            act(pltpu.make_async_copy(source, to, sems.at[i]))
        for i, (start, size) in enumerate(pieces):
            rows = pl.ds(start, size)
            late = outer & is_late(i, len(pieces))

            @pl.when(jnp.logical_not(late))
            def _():
                act(pltpu.make_async_copy(
                    held.at[rows, :], result.at[rows, :], held_sems.at[i]
                ))

            @pl.when(late)
            def _():
                here = (rows, pl.ds(pl.multiple_of(me * depth, 128), depth))
                act(pltpu.make_async_copy(held.at[here], result.at[here], held_sems.at[i]))

    each(lambda copy: copy.start())
    token[...] = jnp.zeros_like(token)
    each(lambda copy: copy.wait())


def flushed(n, done, held):
    vmem, hbm = pl.BlockSpec(memory_space=pltpu.VMEM), pl.BlockSpec(memory_space=pltpu.HBM)
    return pl.pallas_call(
        functools.partial(flush_kernel, n, len(done)),
        out_shape=[jax.ShapeDtypeStruct(x.shape, x.dtype) for x in (*done, held)]
        + [pltpu.VMEM((8, 128), jnp.float32)],
        in_specs=[vmem] * (len(done) + 1),
        out_specs=[hbm] * (len(done) + 1) + [vmem],
        scratch_shapes=[
            pltpu.SemaphoreType.DMA((len(done),)),
            pltpu.SemaphoreType.DMA((len(last_pieces(held.shape[0])),)),
        ],
        compiler_params=pltpu.CompilerParams(vmem_limit_bytes=2**20),
        name="flush",
    )(*done, held)


def lay_out(parts, flat):
    tp, n, _, part = parts.shape
    for row in range(flat.shape[0]):
        cells, at = [], row * 128
        while at < (row + 1) * 128:
            slot, lo = divmod(at, part)
            size = min(part - lo, (row + 1) * 128 - at)
            cells.append(parts[slot % tp, slot // tp, 0:1, lo : lo + size])
            at += size
        flat[row : row + 1, :] = jnp.concatenate(cells, axis=1) if len(cells) > 1 else cells[0]


def tail_kernel(n, tp, depth, held, line, token, tail, norm_out, *scratch):
    lines, norm_flat, send_sem, recv_sem, side_send, side_recv = scratch
    me, my_tp = lax.axis_index("shard"), lax.axis_index("tp")
    pieces = last_pieces(held.shape[0])
    ends = ((1, n - 1), (-1, 0))

    core = lax.rem(lax.axis_index("trial"), 2)
    pl.when((core == 1) & ((me == 0) | (me == n - 1)))(lambda: pl.delay(YIELD_NS))

    barrier = pltpu.get_barrier_semaphore()
    for way, at in ends:
        @pl.when(me == at)
        def _():
            pl.semaphore_signal(
                barrier, inc=1, device_id={"shard": at - way}, device_id_type=MESH
            )
    for t in range(1, tp):
        pl.semaphore_signal(
            barrier, inc=1, device_id={"tp": lax.rem(my_tp + t, tp)}, device_id_type=MESH
        )
    lines[my_tp] = line[...]
    greeted = sum(jnp.where(me == at - way, 1, 0) for way, at in ends) + tp - 1
    pl.when(greeted > 0)(lambda: pl.semaphore_wait(barrier, greeted))

    def each(way, at, away, act):
        for i, (start, size) in enumerate(pieces):
            here = (pl.ds(start, size), pl.ds(0 if way > 0 else depth, (n - 1) * depth))
            slot = (0 if way > 0 else len(pieces)) + i

            @pl.when((me == at - away) & is_late(i, len(pieces)))
            def _():
                act(pltpu.make_async_remote_copy(
                    held.at[here], tail.at[here], send_sem.at[slot], recv_sem.at[slot],
                    device_id={"shard": at}, device_id_type=MESH,
                ))

    def side(t, column):
        return pltpu.make_async_remote_copy(
            line, lines.at[column], side_send.at[t - 1], side_recv.at[t - 1],
            device_id={"tp": lax.rem(my_tp + t, tp)}, device_id_type=MESH,
        )

    for way, at in ends:
        each(way, at, way, lambda copy: copy.start())
    for t in range(1, tp):
        side(t, my_tp).start()
    for t in range(1, tp):
        side(t, lax.rem(my_tp - t + tp, tp)).wait_recv()
    lay_out(lines, norm_flat)
    norm_out[...] = norm_flat[...].astype(jnp.bfloat16)
    for way, at in ends:
        each(way, at, 0, lambda copy: copy.wait_recv())
    for way, at in ends:
        each(way, at, way, lambda copy: copy.wait_send())
    for t in range(1, tp):
        side(t, my_tp).wait_send()


def tailed(n, tp, depth, held, line, token):
    vmem = pl.BlockSpec(memory_space=pltpu.VMEM)
    count = len(last_pieces(held.shape[0]))
    lines = (tp, *line.shape)
    flat = (math.prod(lines) // 128, 128)
    return pl.pallas_call(
        functools.partial(tail_kernel, n, tp, depth),
        out_shape=[pltpu.VMEM(held.shape, held.dtype), pltpu.VMEM(flat, jnp.bfloat16)],
        in_specs=[vmem] * 3,
        out_specs=[vmem] * 2,
        scratch_shapes=[
            pltpu.VMEM(lines, jnp.float32),
            pltpu.VMEM(flat, jnp.float32),
            pltpu.SemaphoreType.DMA((2 * count,)),
            pltpu.SemaphoreType.DMA((2 * count,)),
            pltpu.SemaphoreType.DMA((max(tp - 1, 1),)),
            pltpu.SemaphoreType.DMA((max(tp - 1, 1),)),
        ],
        compiler_params=pltpu.CompilerParams(
            collective_id=1, has_side_effects=True, vmem_limit_bytes=2**20
        ),
        name="tail",
    )(held, line, token)


def close_kernel(n, tail, norm, begun, result, norm_out, sems):
    me = lax.axis_index("shard")
    pieces = last_pieces(tail.shape[0])
    depth = tail.shape[1] // n

    def each(act):
        for at in (0, n - 1):
            for i, (start, size) in enumerate(pieces):
                here = (pl.ds(start, size), pl.ds(0 if at else depth, (n - 1) * depth))

                @pl.when((me == at) & is_late(i, len(pieces)))
                def _():
                    act(pltpu.make_async_copy(tail.at[here], result.at[here], sems.at[i]))
        act(pltpu.make_async_copy(norm, norm_out, sems.at[len(pieces)]))

    each(lambda copy: copy.start())
    each(lambda copy: copy.wait())


def closed(n, tail, norm, begun):
    vmem, hbm = pl.BlockSpec(memory_space=pltpu.VMEM), pl.BlockSpec(memory_space=pltpu.HBM)
    return pl.pallas_call(
        functools.partial(close_kernel, n),
        out_shape=[jax.ShapeDtypeStruct(x.shape, x.dtype) for x in (begun, norm)],
        in_specs=[vmem, vmem, hbm],
        out_specs=[hbm] * 2,
        input_output_aliases={2: 0},
        scratch_shapes=[pltpu.SemaphoreType.DMA((len(last_pieces(tail.shape[0])) + 1,))],
        compiler_params=pltpu.CompilerParams(vmem_limit_bytes=2**20),
        name="close",
    )(tail, norm, begun)


def plain(weights, lows, highs, norm_new):
    serve = []
    for weight, low, high in zip(weights, lows, highs):
        fresh = weight.astype(jnp.float32) + mix_rate * jnp.dot(
            low, high, preferred_element_type=jnp.float32
        )
        serve.append(
            lax.all_gather(fresh.astype(jnp.bfloat16), "shard", axis=0, tiled=True).T
        )
    norm = lax.all_gather(
        norm_new.astype(jnp.bfloat16), ("shard", "tp"), axis=0, tiled=True
    )
    return (*serve, norm)


def on_device(n, tp, wq, lq, hq, wk, lk, hk, wv, lv, hv, norm_train, norm_step):
    weights, lows, highs = (wq, wk, wv), (lq, lk, lv), (hq, hk, hv)
    depth = wq.shape[0]
    if n < 2 or depth % 128 or any(weight.shape[1] % ROWS for weight in weights) or wv.shape[1] < 2 * ROWS:
        return plain(weights, lows, highs, norm_train + norm_step)
    query, key, value, line = gathered(
        n, ROWS, weights, [low.T for low in lows], highs, norm_train, norm_step
    )
    query, key, begun, token = flushed(n, [query, key], value)
    tail, norm = tailed(n, tp, depth, value, line, token)
    value, norm = closed(n, tail, norm, begun)
    return (query, key, value, norm.reshape(-1))


def solution(mesh):
    in_specs = (
        (P(("trial", "shard"), "tp"), P(("trial", "shard"), None), P("trial", "tp")) * 3
        + (P(("trial", "shard", "tp")),) * 2
    )
    out_specs = (P(("trial", "tp"), None),) * 3 + (P("trial"),)
    body = functools.partial(on_device, mesh.shape["shard"], mesh.shape["tp"])
    return jax.shard_map(
        body, mesh=mesh, in_specs=in_specs, out_specs=out_specs, check_vma=False
    )
```

```python
import functools
import math

import jax
import jax.numpy as jnp
from jax import lax
from jax.experimental import pallas as pl
from jax.experimental.pallas import tpu as pltpu
from jax.sharding import PartitionSpec as P

mix_rate = 1.0
MESH = pl.DeviceIdType.MESH
ROWS = 128
PIECE = 1024
LATE = (2, 1)
YIELD_NS = 4000


def cut(width, sizes):
    pieces, at = [], 0
    while at < width:
        size = min(sizes[len(pieces)] if len(pieces) < len(sizes) else PIECE, width - at)
        pieces.append((at, size))
        at += size
    return pieces


def last_pieces(width):
    return cut(width, [width - ROWS, ROWS])


def is_late(index, count):
    core = lax.rem(lax.axis_index("trial"), 2)
    late = [index >= count - x for x in LATE]
    if late[0] == late[1]:
        return late[0]
    return core == (0 if late[0] else 1)


def gather_kernel(n, rows, *refs):
    weights, low_refs, high_refs = refs[0:3], refs[3:6], refs[6:9]
    norms = refs[9:11]
    outs, line = refs[11:14], refs[14]
    staged, lows, highs = refs[15], refs[16:19], refs[19:22]
    (load_sem, small_sem, send_sem, recv_sem, ready,
     train, change, norm_sem, chain_send, chain_recv) = refs[22:]
    me = lax.axis_index("shard")
    depth = staged.shape[1]
    counts = [weight.shape[1] // rows for weight in weights]
    starts = [sum(counts[:i]) for i in range(len(counts))]
    total = sum(counts)
    last = len(counts) - 1
    widths = [weight.shape[1] for weight in weights]
    plan = [cut(widths[0], [rows, 3 * rows]), cut(widths[1], []), last_pieces(widths[2])]
    pieces = [(which, i, *piece) for which in range(3) for i, piece in enumerate(plan[which])]

    def load(which, c):
        return pltpu.make_async_copy(
            weights[which].at[:, pl.ds(pl.multiple_of(c * rows, rows), rows)],
            staged.at[starts[which] + c],
            load_sem.at[starts[which] + c],
        )

    def low_copy(which):
        return pltpu.make_async_copy(low_refs[which], lows[which], small_sem.at[6 + which])

    def high_part(which, part):
        lo, hi = (0, rows) if part == 0 else (rows, highs[which].shape[1])
        here = (slice(None), pl.ds(lo, hi - lo))
        return pltpu.make_async_copy(
            high_refs[which].at[here], highs[which].at[here], small_sem.at[2 * which + part]
        )

    load(0, 0).start()
    low_copy(0).start()
    high_part(0, 0).start()

    barrier = pltpu.get_barrier_semaphore()

    @pl.when(me < n - 1)
    def _():
        pl.semaphore_signal(
            barrier, inc=1, device_id={"shard": jnp.minimum(me + 1, n - 1)},
            device_id_type=MESH,
        )

    @pl.when(me > 0)
    def _():
        pl.semaphore_wait(barrier, 1)
        pl.semaphore_signal(
            ready, inc=1, device_id={"shard": jnp.maximum(me - 1, 0)}, device_id_type=MESH
        )

    norm_loads = [
        pltpu.make_async_copy(norms[0], train, norm_sem.at[0]),
        pltpu.make_async_copy(norms[1], change, norm_sem.at[1]),
    ]

    def load_rest():
        for copy in norm_loads:
            copy.start()
        for which in range(3):
            if which:
                low_copy(which).start()
                high_part(which, 0).start()
            high_part(which, 1).start()

            @pl.loop(0 if which else 1, counts[which])
            def _(c):
                load(which, c).start()

    def block(p, owner):
        which, _, start, size = pieces[p]
        return outs[which].at[
            pl.ds(start, size), pl.ds(pl.multiple_of(owner * depth, 128), depth)
        ]

    def lane(step, way):
        return (0 if way > 0 else 1) * (n - 1) + step

    def ahead(way):
        return {"shard": jnp.clip(me + way, 0, n - 1)}

    def hop(p, step, way, owner):
        here = block(p, owner)
        slot = lane(step, way) * len(pieces) + p
        return pltpu.make_async_remote_copy(
            here, here, send_sem.at[slot], recv_sem.at[slot],
            device_id=ahead(way), device_id_type=MESH,
        )

    def chain(hops, way, owner):
        here = line.at[owner]
        return pltpu.make_async_remote_copy(
            here, here, chain_send.at[lane(hops, way)], chain_recv.at[lane(hops, way)],
            device_id=ahead(way), device_id_type=MESH,
        )

    def end(at, way):
        return at == (n - 1 if way > 0 else 0)

    def sends(step, way):
        owner = me - way * step
        ok = (owner >= 0) & (owner < n) & (me + way >= 0) & (me + way < n)
        return ok, jnp.clip(owner, 0, n - 1)

    def arrives(step, way):
        owner = me - way * (step + 1)
        return (owner >= 0) & (owner < n), jnp.clip(owner, 0, n - 1)

    def now(p, at, way):
        which, i = pieces[p][:2]
        if which != last:
            return True
        return jnp.logical_not(is_late(i, len(plan[last])) & end(at, way))

    def send(p, way):
        ok, owner = sends(0, way)
        ok = ok & now(p, me + way, way)
        pl.when(ok)(lambda: hop(p, 0, way, owner).start())

    def merge(which, c):
        load(which, c).wait()
        high = highs[which][:, pl.ds(pl.multiple_of(c * rows, rows), rows)]
        fresh = staged[starts[which] + c].T.astype(jnp.float32) + mix_rate * lax.dot_general(
            high, lows[which][...], (((0,), (0,)), ((), ())),
            preferred_element_type=jnp.float32,
        )
        outs[which][
            pl.ds(pl.multiple_of(c * rows, rows), rows),
            pl.ds(pl.multiple_of(me * depth, 128), depth),
        ] = fresh.astype(jnp.bfloat16)

    low_copy(0).wait()
    high_part(0, 0).wait()
    merge(0, 0)

    send(0, -1)
    pl.when(me < n - 1)(lambda: pl.semaphore_wait(ready, 1))
    send(0, 1)
    load_rest()
    for copy in norm_loads:
        copy.wait()
    line[me, 0, :] = train[...] + change[...]
    for way in (1, -1):
        ok, owner = sends(0, way)
        pl.when(ok)(lambda: chain(0, way, owner).start())
    for p, (which, i, start, size) in enumerate(pieces):
        if p == 0:
            continue
        if i == 0:
            low_copy(which).wait()
            high_part(which, 0).wait()
        if i == 0 or p == 1:
            high_part(which, 1).wait()
        pl.loop(start // rows, (start + size) // rows)(functools.partial(merge, which))
        send(p, -1)
        send(p, 1)

    def pass_norm(step):
        for way in (1, -1):
            ok, owner = arrives(step, way)
            further = ok & (me + way >= 0) & (me + way < n)
            pl.when(ok)(lambda: chain(step, way, owner).wait_recv())
            if step < n - 2:
                pl.when(further)(lambda: chain(step + 1, way, owner).start())

    def pass_on(p, step):
        for way in (1, -1):
            ok, owner = arrives(step, way)
            further = ok & (me + way >= 0) & (me + way < n) & now(p, me + way, way)
            ok = ok & now(p, me, way)
            pl.when(ok)(lambda: hop(p, step, way, owner).wait_recv())
            if step < n - 2:
                pl.when(further)(lambda: hop(p, step + 1, way, owner).start())

    for step in range(n - 1):
        pass_norm(step)
        for p in range(len(pieces)):
            pass_on(p, step)

    def sent(p, step):
        for way in (1, -1):
            ok, owner = sends(step, way)
            ok = ok & now(p, me + way, way)
            pl.when(ok)(lambda: hop(p, step, way, owner).wait_send())

    for step in range(n - 1):
        for way in (1, -1):
            ok, owner = sends(step, way)
            pl.when(ok)(lambda: chain(step, way, owner).wait_send())
        for p in range(len(pieces)):
            sent(p, step)


def gathered(n, rows, weights, lows, highs, train, step):
    depth = weights[0].shape[0]
    total = sum(weight.shape[1] // rows for weight in weights)
    vmem, hbm = pl.BlockSpec(memory_space=pltpu.VMEM), pl.BlockSpec(memory_space=pltpu.HBM)
    return pl.pallas_call(
        functools.partial(gather_kernel, n, rows),
        out_shape=[pltpu.VMEM((weight.shape[1], n * depth), jnp.bfloat16) for weight in weights]
        + [pltpu.VMEM((n, 1, train.shape[0]), jnp.float32)],
        in_specs=[hbm] * 11,
        out_specs=[vmem] * 4,
        scratch_shapes=[
            pltpu.VMEM((total, depth, rows), jnp.bfloat16),
            *[pltpu.VMEM(x.shape, x.dtype) for x in (*lows, *highs)],
            pltpu.SemaphoreType.DMA((total,)),
            pltpu.SemaphoreType.DMA((9,)),
            pltpu.SemaphoreType.DMA((2 * (n - 1) * total,)),
            pltpu.SemaphoreType.DMA((2 * (n - 1) * total,)),
            pltpu.SemaphoreType.REGULAR,
            pltpu.VMEM(train.shape, jnp.float32),
            pltpu.VMEM(step.shape, jnp.float32),
            pltpu.SemaphoreType.DMA((2,)),
            pltpu.SemaphoreType.DMA((2 * (n - 1),)),
            pltpu.SemaphoreType.DMA((2 * (n - 1),)),
        ],
        compiler_params=pltpu.CompilerParams(
            collective_id=0, has_side_effects=True, vmem_limit_bytes=47 * 2**20
        ),
        name="gather",
    )(*weights, *lows, *highs, train, step)


def flush_kernel(n, count, *refs):
    sources, held = refs[:count], refs[count]
    results, result = refs[count + 1 : 2 * count + 1], refs[2 * count + 1]
    token, sems, held_sems = refs[2 * count + 2 :]
    me = lax.axis_index("shard")
    depth = held.shape[1] // n
    pieces = last_pieces(held.shape[0])
    outer = (me == 0) | (me == n - 1)

    def each(act):
        for i, (source, to) in enumerate(zip(sources, results)):
            act(pltpu.make_async_copy(source, to, sems.at[i]))
        for i, (start, size) in enumerate(pieces):
            rows = pl.ds(start, size)
            late = outer & is_late(i, len(pieces))

            @pl.when(jnp.logical_not(late))
            def _():
                act(pltpu.make_async_copy(
                    held.at[rows, :], result.at[rows, :], held_sems.at[i]
                ))

            @pl.when(late)
            def _():
                here = (rows, pl.ds(pl.multiple_of(me * depth, 128), depth))
                act(pltpu.make_async_copy(held.at[here], result.at[here], held_sems.at[i]))

    each(lambda copy: copy.start())
    token[...] = jnp.zeros_like(token)
    each(lambda copy: copy.wait())


def flushed(n, done, held):
    vmem, hbm = pl.BlockSpec(memory_space=pltpu.VMEM), pl.BlockSpec(memory_space=pltpu.HBM)
    return pl.pallas_call(
        functools.partial(flush_kernel, n, len(done)),
        out_shape=[jax.ShapeDtypeStruct(x.shape, x.dtype) for x in (*done, held)]
        + [pltpu.VMEM((8, 128), jnp.float32)],
        in_specs=[vmem] * (len(done) + 1),
        out_specs=[hbm] * (len(done) + 1) + [vmem],
        scratch_shapes=[
            pltpu.SemaphoreType.DMA((len(done),)),
            pltpu.SemaphoreType.DMA((len(last_pieces(held.shape[0])),)),
        ],
        compiler_params=pltpu.CompilerParams(vmem_limit_bytes=2**20),
        name="flush",
    )(*done, held)


def lay_out(parts, flat):
    tp, n, _, part = parts.shape
    for row in range(flat.shape[0]):
        cells, at = [], row * 128
        while at < (row + 1) * 128:
            slot, lo = divmod(at, part)
            size = min(part - lo, (row + 1) * 128 - at)
            cells.append(parts[slot % tp, slot // tp, 0:1, lo : lo + size])
            at += size
        flat[row : row + 1, :] = jnp.concatenate(cells, axis=1) if len(cells) > 1 else cells[0]


def tail_kernel(n, tp, depth, held, line, token, tail, norm_out, *scratch):
    lines, norm_flat, send_sem, recv_sem, side_send, side_recv = scratch
    me, my_tp = lax.axis_index("shard"), lax.axis_index("tp")
    pieces = last_pieces(held.shape[0])
    ends = ((1, n - 1), (-1, 0))

    core = lax.rem(lax.axis_index("trial"), 2)
    pl.when((core == 1) & ((me == 0) | (me == n - 1)))(lambda: pl.delay(YIELD_NS))

    barrier = pltpu.get_barrier_semaphore()
    for way, at in ends:
        @pl.when(me == at)
        def _():
            pl.semaphore_signal(
                barrier, inc=1, device_id={"shard": at - way}, device_id_type=MESH
            )
    for t in range(1, tp):
        pl.semaphore_signal(
            barrier, inc=1, device_id={"tp": lax.rem(my_tp + t, tp)}, device_id_type=MESH
        )
    lines[my_tp] = line[...]
    greeted = sum(jnp.where(me == at - way, 1, 0) for way, at in ends) + tp - 1
    pl.when(greeted > 0)(lambda: pl.semaphore_wait(barrier, greeted))

    def each(way, at, away, act):
        for i, (start, size) in enumerate(pieces):
            here = (pl.ds(start, size), pl.ds(0 if way > 0 else depth, (n - 1) * depth))
            slot = (0 if way > 0 else len(pieces)) + i

            @pl.when((me == at - away) & is_late(i, len(pieces)))
            def _():
                act(pltpu.make_async_remote_copy(
                    held.at[here], tail.at[here], send_sem.at[slot], recv_sem.at[slot],
                    device_id={"shard": at}, device_id_type=MESH,
                ))

    def side(t, column):
        return pltpu.make_async_remote_copy(
            line, lines.at[column], side_send.at[t - 1], side_recv.at[t - 1],
            device_id={"tp": lax.rem(my_tp + t, tp)}, device_id_type=MESH,
        )

    for way, at in ends:
        each(way, at, way, lambda copy: copy.start())
    for t in range(1, tp):
        side(t, my_tp).start()
    for t in range(1, tp):
        side(t, lax.rem(my_tp - t + tp, tp)).wait_recv()
    lay_out(lines, norm_flat)
    norm_out[...] = norm_flat[...].astype(jnp.bfloat16)
    for way, at in ends:
        each(way, at, 0, lambda copy: copy.wait_recv())
    for way, at in ends:
        each(way, at, way, lambda copy: copy.wait_send())
    for t in range(1, tp):
        side(t, my_tp).wait_send()


def tailed(n, tp, depth, held, line, token):
    vmem = pl.BlockSpec(memory_space=pltpu.VMEM)
    count = len(last_pieces(held.shape[0]))
    lines = (tp, *line.shape)
    flat = (math.prod(lines) // 128, 128)
    return pl.pallas_call(
        functools.partial(tail_kernel, n, tp, depth),
        out_shape=[pltpu.VMEM(held.shape, held.dtype), pltpu.VMEM(flat, jnp.bfloat16)],
        in_specs=[vmem] * 3,
        out_specs=[vmem] * 2,
        scratch_shapes=[
            pltpu.VMEM(lines, jnp.float32),
            pltpu.VMEM(flat, jnp.float32),
            pltpu.SemaphoreType.DMA((2 * count,)),
            pltpu.SemaphoreType.DMA((2 * count,)),
            pltpu.SemaphoreType.DMA((max(tp - 1, 1),)),
            pltpu.SemaphoreType.DMA((max(tp - 1, 1),)),
        ],
        compiler_params=pltpu.CompilerParams(
            collective_id=1, has_side_effects=True, vmem_limit_bytes=2**20
        ),
        name="tail",
    )(held, line, token)


def close_kernel(n, tail, norm, begun, result, norm_out, sems):
    me = lax.axis_index("shard")
    pieces = last_pieces(tail.shape[0])
    depth = tail.shape[1] // n

    def each(act):
        for at in (0, n - 1):
            for i, (start, size) in enumerate(pieces):
                here = (pl.ds(start, size), pl.ds(0 if at else depth, (n - 1) * depth))

                @pl.when((me == at) & is_late(i, len(pieces)))
                def _():
                    act(pltpu.make_async_copy(tail.at[here], result.at[here], sems.at[i]))
        act(pltpu.make_async_copy(norm, norm_out, sems.at[len(pieces)]))

    each(lambda copy: copy.start())
    each(lambda copy: copy.wait())


def closed(n, tail, norm, begun):
    vmem, hbm = pl.BlockSpec(memory_space=pltpu.VMEM), pl.BlockSpec(memory_space=pltpu.HBM)
    return pl.pallas_call(
        functools.partial(close_kernel, n),
        out_shape=[jax.ShapeDtypeStruct(x.shape, x.dtype) for x in (begun, norm)],
        in_specs=[vmem, vmem, hbm],
        out_specs=[hbm] * 2,
        input_output_aliases={2: 0},
        scratch_shapes=[pltpu.SemaphoreType.DMA((len(last_pieces(tail.shape[0])) + 1,))],
        compiler_params=pltpu.CompilerParams(vmem_limit_bytes=2**20),
        name="close",
    )(tail, norm, begun)


def plain(weights, lows, highs, norm_new):
    serve = []
    for weight, low, high in zip(weights, lows, highs):
        fresh = weight.astype(jnp.float32) + mix_rate * jnp.dot(
            low, high, preferred_element_type=jnp.float32
        )
        serve.append(
            lax.all_gather(fresh.astype(jnp.bfloat16), "shard", axis=0, tiled=True).T
        )
    norm = lax.all_gather(
        norm_new.astype(jnp.bfloat16), ("shard", "tp"), axis=0, tiled=True
    )
    return (*serve, norm)


def on_device(n, tp, wq, lq, hq, wk, lk, hk, wv, lv, hv, norm_train, norm_step):
    weights, lows, highs = (wq, wk, wv), (lq, lk, lv), (hq, hk, hv)
    depth = wq.shape[0]
    if n < 2 or depth % 128 or any(w.shape[1] % ROWS or w.shape[1] < 2 * ROWS for w in weights):
        return plain(weights, lows, highs, norm_train + norm_step)
    query, key, value, line = gathered(
        n, ROWS, weights, [low.T for low in lows], highs, norm_train, norm_step
    )
    query, key, begun, token = flushed(n, [query, key], value)
    tail, norm = tailed(n, tp, depth, value, line, token)
    value, norm = closed(n, tail, norm, begun)
    return (query, key, value, norm.reshape(-1))


def solution(mesh):
    in_specs = (
        (P(("trial", "shard"), "tp"), P(("trial", "shard"), None), P("trial", "tp")) * 3
        + (P(("trial", "shard", "tp")),) * 2
    )
    out_specs = (P(("trial", "tp"), None),) * 3 + (P("trial"),)
    body = functools.partial(on_device, mesh.shape["shard"], mesh.shape["tp"])
    return jax.shard_map(
        body, mesh=mesh, in_specs=in_specs, out_specs=out_specs, check_vma=False
    )
```

```python
import functools
import math

import jax
import jax.numpy as jnp
from jax import lax
from jax.experimental import pallas as pl
from jax.experimental.pallas import tpu as pltpu
from jax.sharding import PartitionSpec as P

mix_rate = 1.0
MESH = pl.DeviceIdType.MESH
ROWS = 128
PIECE = 2048
LATE = (2, 1)
YIELD_NS = (2200, 1800)
SHARE = 8
AIDED = (1, 0)
HELPERS = ((3, 0), (1, 1))


def cut(width, sizes):
    pieces, at = [], 0
    while at < width:
        size = min(sizes[len(pieces)] if len(pieces) < len(sizes) else PIECE, width - at)
        pieces.append((at, size))
        at += size
    return pieces


def last_pieces(width):
    return cut(width, [width - ROWS, ROWS])


def is_late(index, count):
    core = lax.rem(lax.axis_index("trial"), 2)
    late = [index >= count - x for x in LATE]
    if late[0] == late[1]:
        return late[0]
    return core == (0 if late[0] else 1)


def gather_kernel(n, rows, *refs):
    weights, low_refs, high_refs = refs[0:3], refs[3:6], refs[6:9]
    norms = refs[9:11]
    outs, line = refs[11:14], refs[14]
    staged, lows, highs = refs[15], refs[16:19], refs[19:22]
    (load_sem, small_sem, send_sem, recv_sem, ready,
     train, change, norm_sem, chain_send, chain_recv) = refs[22:]
    me = lax.axis_index("shard")
    depth = staged.shape[1]
    counts = [weight.shape[1] // rows for weight in weights]
    starts = [sum(counts[:i]) for i in range(len(counts))]
    total = sum(counts)
    last = len(counts) - 1
    widths = [weight.shape[1] for weight in weights]
    plan = [cut(widths[0], [rows, 3 * rows]), cut(widths[1], []), last_pieces(widths[2])]
    pieces = [(which, i, *piece) for which in range(3) for i, piece in enumerate(plan[which])]

    def load(which, c):
        return pltpu.make_async_copy(
            weights[which].at[:, pl.ds(pl.multiple_of(c * rows, rows), rows)],
            staged.at[starts[which] + c],
            load_sem.at[starts[which] + c],
        )

    def low_copy(which):
        return pltpu.make_async_copy(low_refs[which], lows[which], small_sem.at[6 + which])

    def high_part(which, part):
        lo, hi = (0, rows) if part == 0 else (rows, highs[which].shape[1])
        here = (slice(None), pl.ds(lo, hi - lo))
        return pltpu.make_async_copy(
            high_refs[which].at[here], highs[which].at[here], small_sem.at[2 * which + part]
        )

    load(0, 0).start()
    low_copy(0).start()
    high_part(0, 0).start()

    barrier = pltpu.get_barrier_semaphore()

    @pl.when(me < n - 1)
    def _():
        pl.semaphore_signal(
            barrier, inc=1, device_id={"shard": jnp.minimum(me + 1, n - 1)},
            device_id_type=MESH,
        )

    @pl.when(me > 0)
    def _():
        pl.semaphore_wait(barrier, 1)
        pl.semaphore_signal(
            ready, inc=1, device_id={"shard": jnp.maximum(me - 1, 0)}, device_id_type=MESH
        )

    norm_loads = [
        pltpu.make_async_copy(norms[0], train, norm_sem.at[0]),
        pltpu.make_async_copy(norms[1], change, norm_sem.at[1]),
    ]

    def load_rest():
        for copy in norm_loads:
            copy.start()
        for which in range(3):
            if which:
                low_copy(which).start()
                high_part(which, 0).start()
            high_part(which, 1).start()

            @pl.loop(0 if which else 1, counts[which])
            def _(c):
                load(which, c).start()

    def block(p, owner):
        which, _, start, size = pieces[p]
        return outs[which].at[
            pl.ds(start, size), pl.ds(pl.multiple_of(owner * depth, 128), depth)
        ]

    def lane(step, way):
        return (0 if way > 0 else 1) * (n - 1) + step

    def ahead(way):
        return {"shard": jnp.clip(me + way, 0, n - 1)}

    def hop(p, step, way, owner):
        here = block(p, owner)
        slot = lane(step, way) * len(pieces) + p
        return pltpu.make_async_remote_copy(
            here, here, send_sem.at[slot], recv_sem.at[slot],
            device_id=ahead(way), device_id_type=MESH,
        )

    def chain(hops, way, owner):
        here = line.at[owner]
        return pltpu.make_async_remote_copy(
            here, here, chain_send.at[lane(hops, way)], chain_recv.at[lane(hops, way)],
            device_id=ahead(way), device_id_type=MESH,
        )

    def end(at, way):
        return at == (n - 1 if way > 0 else 0)

    def sends(step, way):
        owner = me - way * step
        ok = (owner >= 0) & (owner < n) & (me + way >= 0) & (me + way < n)
        return ok, jnp.clip(owner, 0, n - 1)

    def arrives(step, way):
        owner = me - way * (step + 1)
        return (owner >= 0) & (owner < n), jnp.clip(owner, 0, n - 1)

    def now(p, at, way):
        which, i = pieces[p][:2]
        if which != last:
            return True
        return jnp.logical_not(is_late(i, len(plan[last])) & end(at, way))

    def send(p, way):
        ok, owner = sends(0, way)
        ok = ok & now(p, me + way, way)
        pl.when(ok)(lambda: hop(p, 0, way, owner).start())

    def merge(which, c):
        load(which, c).wait()
        high = highs[which][:, pl.ds(pl.multiple_of(c * rows, rows), rows)]
        fresh = staged[starts[which] + c].T.astype(jnp.float32) + mix_rate * lax.dot_general(
            high, lows[which][...], (((0,), (0,)), ((), ())),
            preferred_element_type=jnp.float32,
        )
        outs[which][
            pl.ds(pl.multiple_of(c * rows, rows), rows),
            pl.ds(pl.multiple_of(me * depth, 128), depth),
        ] = fresh.astype(jnp.bfloat16)

    low_copy(0).wait()
    high_part(0, 0).wait()
    merge(0, 0)

    send(0, -1)
    pl.when(me < n - 1)(lambda: pl.semaphore_wait(ready, 1))
    send(0, 1)
    load_rest()
    for copy in norm_loads:
        copy.wait()
    line[me, 0, :] = train[...] + change[...]
    for way in (1, -1):
        ok, owner = sends(0, way)
        pl.when(ok)(lambda: chain(0, way, owner).start())
    for p, (which, i, start, size) in enumerate(pieces):
        if p == 0:
            continue
        if i == 0:
            low_copy(which).wait()
            high_part(which, 0).wait()
        if i == 0 or p == 1:
            high_part(which, 1).wait()
        pl.loop(start // rows, (start + size) // rows)(functools.partial(merge, which))
        send(p, -1)
        send(p, 1)

    def pass_norm(step):
        for way in (1, -1):
            ok, owner = arrives(step, way)
            further = ok & (me + way >= 0) & (me + way < n)
            pl.when(ok)(lambda: chain(step, way, owner).wait_recv())
            if step < n - 2:
                pl.when(further)(lambda: chain(step + 1, way, owner).start())

    def pass_on(p, step):
        for way in (1, -1):
            ok, owner = arrives(step, way)
            further = ok & (me + way >= 0) & (me + way < n) & now(p, me + way, way)
            ok = ok & now(p, me, way)
            pl.when(ok)(lambda: hop(p, step, way, owner).wait_recv())
            if step < n - 2:
                pl.when(further)(lambda: hop(p, step + 1, way, owner).start())

    for step in range(n - 1):
        pass_norm(step)
        for p in range(len(pieces)):
            pass_on(p, step)

    def sent(p, step):
        for way in (1, -1):
            ok, owner = sends(step, way)
            ok = ok & now(p, me + way, way)
            pl.when(ok)(lambda: hop(p, step, way, owner).wait_send())

    for step in range(n - 1):
        for way in (1, -1):
            ok, owner = sends(step, way)
            pl.when(ok)(lambda: chain(step, way, owner).wait_send())
        for p in range(len(pieces)):
            sent(p, step)


def gathered(n, rows, weights, lows, highs, train, step):
    depth = weights[0].shape[0]
    total = sum(weight.shape[1] // rows for weight in weights)
    vmem, hbm = pl.BlockSpec(memory_space=pltpu.VMEM), pl.BlockSpec(memory_space=pltpu.HBM)
    return pl.pallas_call(
        functools.partial(gather_kernel, n, rows),
        out_shape=[pltpu.VMEM((weight.shape[1], n * depth), jnp.bfloat16) for weight in weights]
        + [pltpu.VMEM((n, 1, train.shape[0]), jnp.float32)],
        in_specs=[hbm] * 11,
        out_specs=[vmem] * 4,
        scratch_shapes=[
            pltpu.VMEM((total, depth, rows), jnp.bfloat16),
            *[pltpu.VMEM(x.shape, x.dtype) for x in (*lows, *highs)],
            pltpu.SemaphoreType.DMA((total,)),
            pltpu.SemaphoreType.DMA((9,)),
            pltpu.SemaphoreType.DMA((2 * (n - 1) * total,)),
            pltpu.SemaphoreType.DMA((2 * (n - 1) * total,)),
            pltpu.SemaphoreType.REGULAR,
            pltpu.VMEM(train.shape, jnp.float32),
            pltpu.VMEM(step.shape, jnp.float32),
            pltpu.SemaphoreType.DMA((2,)),
            pltpu.SemaphoreType.DMA((2 * (n - 1),)),
            pltpu.SemaphoreType.DMA((2 * (n - 1),)),
        ],
        compiler_params=pltpu.CompilerParams(
            collective_id=0, has_side_effects=True, vmem_limit_bytes=47 * 2**20
        ),
        name="gather",
    )(*weights, *lows, *highs, train, step)


def flush_kernel(n, count, *refs):
    sources, held = refs[:count], refs[count]
    results, result = refs[count + 1 : 2 * count + 1], refs[2 * count + 1]
    token, sems, held_sems = refs[2 * count + 2 :]
    me = lax.axis_index("shard")
    depth = held.shape[1] // n
    pieces = last_pieces(held.shape[0])
    outer = (me == 0) | (me == n - 1)

    def each(act):
        for i, (source, to) in enumerate(zip(sources, results)):
            act(pltpu.make_async_copy(source, to, sems.at[i]))
        for i, (start, size) in enumerate(pieces):
            rows = pl.ds(start, size)
            late = outer & is_late(i, len(pieces))

            @pl.when(jnp.logical_not(late))
            def _():
                act(pltpu.make_async_copy(
                    held.at[rows, :], result.at[rows, :], held_sems.at[i]
                ))

            @pl.when(late)
            def _():
                here = (rows, pl.ds(pl.multiple_of(me * depth, 128), depth))
                act(pltpu.make_async_copy(held.at[here], result.at[here], held_sems.at[i]))

    each(lambda copy: copy.start())
    token[...] = jnp.zeros_like(token)
    each(lambda copy: copy.wait())


def flushed(n, done, held):
    vmem, hbm = pl.BlockSpec(memory_space=pltpu.VMEM), pl.BlockSpec(memory_space=pltpu.HBM)
    return pl.pallas_call(
        functools.partial(flush_kernel, n, len(done)),
        out_shape=[jax.ShapeDtypeStruct(x.shape, x.dtype) for x in (*done, held)]
        + [pltpu.VMEM((8, 128), jnp.float32)],
        in_specs=[vmem] * (len(done) + 1),
        out_specs=[hbm] * (len(done) + 1) + [vmem],
        scratch_shapes=[
            pltpu.SemaphoreType.DMA((len(done),)),
            pltpu.SemaphoreType.DMA((len(last_pieces(held.shape[0])),)),
        ],
        compiler_params=pltpu.CompilerParams(vmem_limit_bytes=2**20),
        name="flush",
    )(*done, held)


def lay_out(parts, flat):
    tp, n, _, part = parts.shape
    for row in range(flat.shape[0]):
        cells, at = [], row * 128
        while at < (row + 1) * 128:
            slot, lo = divmod(at, part)
            size = min(part - lo, (row + 1) * 128 - at)
            cells.append(parts[slot % tp, slot // tp, 0:1, lo : lo + size])
            at += size
        flat[row : row + 1, :] = jnp.concatenate(cells, axis=1) if len(cells) > 1 else cells[0]


def tail_kernel(n, tp, helpers, depth, held, line, token, tail, norm_out, *scratch):
    lines, norm_flat, relay, send_sem, recv_sem, side_send, side_recv, aid_send, aid_recv = scratch
    trial = lax.axis_index("trial")
    me, my_tp = lax.axis_index("shard"), lax.axis_index("tp")
    pieces = last_pieces(held.shape[0])
    ends = ((1, n - 1), (-1, 0))

    def at_place(place, shard):
        return (trial == place[0]) & (my_tp == place[1]) & (me == shard)

    def device(place, shard):
        return {"trial": place[0], "tp": place[1], "shard": shard}

    def legs(h):
        start = held.shape[0] - (h + 1) * SHARE
        rows = (pl.ds(start, SHARE), pl.ds(depth, (n - 1) * depth))
        return (
            ((AIDED, 1), (helpers[h], 1), held.at[rows], relay),
            ((helpers[h], 1), (helpers[h], 0), relay, relay),
            ((helpers[h], 0), (AIDED, 0), relay, tail.at[rows]),
        )

    def leg(h, k):
        origin, goal, source, target = legs(h)[k]
        return origin, goal, pltpu.make_async_remote_copy(
            source, target, aid_send.at[3 * h + k], aid_recv.at[3 * h + k],
            device_id=device(*goal), device_id_type=MESH,
        )

    def start_leg(h, k):
        origin, _, copy = leg(h, k)

        @pl.when(at_place(*origin))
        def _():
            if k:
                leg(h, k - 1)[2].wait_recv()
            copy.start()

    barrier = pltpu.get_barrier_semaphore()
    for way, at in ends:
        @pl.when(me == at)
        def _():
            pl.semaphore_signal(
                barrier, inc=1, device_id={"shard": at - way}, device_id_type=MESH
            )
    for t in range(1, tp):
        pl.semaphore_signal(
            barrier, inc=1, device_id={"tp": lax.rem(my_tp + t, tp)}, device_id_type=MESH
        )
    lines[my_tp] = line[...]
    greeted = sum(jnp.where(me == at - way, 1, 0) for way, at in ends) + tp - 1
    for h in range(len(helpers)):
        for k in range(3):
            origin, goal = legs(h)[k][:2]
            greeted = greeted + jnp.where(at_place(*origin), 1, 0)

            @pl.when(at_place(*goal))
            def _():
                pl.semaphore_signal(
                    barrier, inc=1, device_id=device(*origin), device_id_type=MESH
                )
    pl.when(greeted > 0)(lambda: pl.semaphore_wait(barrier, greeted))

    def each(way, at, away, act):
        for i, (start, size) in enumerate(pieces):
            slot = (0 if way > 0 else len(pieces)) + i
            own = size - len(helpers) * SHARE if i == len(pieces) - 1 else size
            parts = [(start, own, slot)]
            if own < size:
                parts.append((start + own, size - own, 2 * len(pieces) + (0 if way > 0 else 1)))
            for part, (lo, rows, sem) in enumerate(parts):
                here = (pl.ds(lo, rows), pl.ds(0 if way > 0 else depth, (n - 1) * depth))
                ok = (me == at - away) & is_late(i, len(pieces))
                if part and way < 0:
                    ok = ok & jnp.logical_not((trial == AIDED[0]) & (my_tp == AIDED[1]))

                @pl.when(ok)
                def _():
                    act(pltpu.make_async_remote_copy(
                        held.at[here], tail.at[here], send_sem.at[sem], recv_sem.at[sem],
                        device_id={"shard": at}, device_id_type=MESH,
                    ))

    def side(t, column):
        return pltpu.make_async_remote_copy(
            line, lines.at[column], side_send.at[t - 1], side_recv.at[t - 1],
            device_id={"tp": lax.rem(my_tp + t, tp)}, device_id_type=MESH,
        )

    late_core = (lax.rem(trial, 2) == 1) & ((me == 1) | (me == n - 2))
    for h in range(len(helpers)):
        start_leg(h, 0)
    pl.when(late_core)(lambda: pl.delay(YIELD_NS[0]))
    for h in range(len(helpers)):
        start_leg(h, 1)
    pl.when(late_core)(lambda: pl.delay(YIELD_NS[1]))
    for way, at in ends:
        each(way, at, way, lambda copy: copy.start())
    for t in range(1, tp):
        side(t, my_tp).start()
    for t in range(1, tp):
        side(t, lax.rem(my_tp - t + tp, tp)).wait_recv()
    for h in range(len(helpers)):
        start_leg(h, 2)
    lay_out(lines, norm_flat)
    norm_out[...] = norm_flat[...].astype(jnp.bfloat16)
    for way, at in ends:
        each(way, at, 0, lambda copy: copy.wait_recv())
    for way, at in ends:
        each(way, at, way, lambda copy: copy.wait_send())
    for t in range(1, tp):
        side(t, my_tp).wait_send()
    for h in range(len(helpers)):
        pl.when(at_place(AIDED, 0))(lambda: leg(h, 2)[2].wait_recv())
        for k in range(3):
            origin, _, copy = leg(h, k)
            pl.when(at_place(*origin))(copy.wait_send)


def tailed(n, tp, helpers, depth, held, line, token):
    vmem = pl.BlockSpec(memory_space=pltpu.VMEM)
    count = len(last_pieces(held.shape[0]))
    lines = (tp, *line.shape)
    flat = (math.prod(lines) // 128, 128)
    return pl.pallas_call(
        functools.partial(tail_kernel, n, tp, helpers, depth),
        out_shape=[pltpu.VMEM(held.shape, held.dtype), pltpu.VMEM(flat, jnp.bfloat16)],
        in_specs=[vmem] * 3,
        out_specs=[vmem] * 2,
        scratch_shapes=[
            pltpu.VMEM(lines, jnp.float32),
            pltpu.VMEM(flat, jnp.float32),
            pltpu.VMEM((SHARE, (n - 1) * depth), jnp.bfloat16),
            pltpu.SemaphoreType.DMA((2 * count + 2,)),
            pltpu.SemaphoreType.DMA((2 * count + 2,)),
            pltpu.SemaphoreType.DMA((max(tp - 1, 1),)),
            pltpu.SemaphoreType.DMA((max(tp - 1, 1),)),
            pltpu.SemaphoreType.DMA((max(3 * len(helpers), 1),)),
            pltpu.SemaphoreType.DMA((max(3 * len(helpers), 1),)),
        ],
        compiler_params=pltpu.CompilerParams(
            collective_id=1, has_side_effects=True, vmem_limit_bytes=2**20
        ),
        name="tail",
    )(held, line, token)


def close_kernel(n, tail, norm, begun, result, norm_out, sems):
    me = lax.axis_index("shard")
    pieces = last_pieces(tail.shape[0])
    depth = tail.shape[1] // n

    def each(act):
        for at in (0, n - 1):
            for i, (start, size) in enumerate(pieces):
                here = (pl.ds(start, size), pl.ds(0 if at else depth, (n - 1) * depth))

                @pl.when((me == at) & is_late(i, len(pieces)))
                def _():
                    act(pltpu.make_async_copy(tail.at[here], result.at[here], sems.at[i]))
        act(pltpu.make_async_copy(norm, norm_out, sems.at[len(pieces)]))

    each(lambda copy: copy.start())
    each(lambda copy: copy.wait())


def closed(n, tail, norm, begun):
    vmem, hbm = pl.BlockSpec(memory_space=pltpu.VMEM), pl.BlockSpec(memory_space=pltpu.HBM)
    return pl.pallas_call(
        functools.partial(close_kernel, n),
        out_shape=[jax.ShapeDtypeStruct(x.shape, x.dtype) for x in (begun, norm)],
        in_specs=[vmem, vmem, hbm],
        out_specs=[hbm] * 2,
        input_output_aliases={2: 0},
        scratch_shapes=[pltpu.SemaphoreType.DMA((len(last_pieces(tail.shape[0])) + 1,))],
        compiler_params=pltpu.CompilerParams(vmem_limit_bytes=2**20),
        name="close",
    )(tail, norm, begun)


def plain(weights, lows, highs, norm_new):
    serve = []
    for weight, low, high in zip(weights, lows, highs):
        fresh = weight.astype(jnp.float32) + mix_rate * jnp.dot(
            low, high, preferred_element_type=jnp.float32
        )
        serve.append(
            lax.all_gather(fresh.astype(jnp.bfloat16), "shard", axis=0, tiled=True).T
        )
    norm = lax.all_gather(
        norm_new.astype(jnp.bfloat16), ("shard", "tp"), axis=0, tiled=True
    )
    return (*serve, norm)


def on_device(trials, n, tp, wq, lq, hq, wk, lk, hk, wv, lv, hv, norm_train, norm_step):
    weights, lows, highs = (wq, wk, wv), (lq, lk, lv), (hq, hk, hv)
    depth = wq.shape[0]
    if n < 2 or depth % 128 or any(w.shape[1] % ROWS or w.shape[1] < 2 * ROWS for w in weights):
        return plain(weights, lows, highs, norm_train + norm_step)
    query, key, value, line = gathered(
        n, ROWS, weights, [low.T for low in lows], highs, norm_train, norm_step
    )
    query, key, begun, token = flushed(n, [query, key], value)
    helpers = [place for place in HELPERS if place[0] < trials and place[1] < tp]
    tail, norm = tailed(n, tp, helpers, depth, value, line, token)
    value, norm = closed(n, tail, norm, begun)
    return (query, key, value, norm.reshape(-1))


def solution(mesh):
    in_specs = (
        (P(("trial", "shard"), "tp"), P(("trial", "shard"), None), P("trial", "tp")) * 3
        + (P(("trial", "shard", "tp")),) * 2
    )
    out_specs = (P(("trial", "tp"), None),) * 3 + (P("trial"),)
    body = functools.partial(on_device, *(mesh.shape[axis] for axis in ("trial", "shard", "tp")))
    return jax.shard_map(
        body, mesh=mesh, in_specs=in_specs, out_specs=out_specs, check_vma=False
    )
```

```python
import functools
import math

import jax
import jax.numpy as jnp
from jax import lax
from jax.experimental import pallas as pl
from jax.experimental.pallas import tpu as pltpu
from jax.sharding import PartitionSpec as P

mix_rate = 1.0
MESH = pl.DeviceIdType.MESH
ROWS = 128
PIECE = 2048
LATE = (2, 1)
YIELD_NS = 3200


def cut(width, sizes):
    pieces, at = [], 0
    while at < width:
        size = min(sizes[len(pieces)] if len(pieces) < len(sizes) else PIECE, width - at)
        pieces.append((at, size))
        at += size
    return pieces


def last_pieces(width):
    return cut(width, [width - ROWS // 2, ROWS // 2])


def is_late(index, count):
    core = lax.rem(lax.axis_index("trial"), 2)
    late = [index >= count - x for x in LATE]
    if late[0] == late[1]:
        return late[0]
    return core == (0 if late[0] else 1)


def gather_kernel(n, rows, *refs):
    weights, low_refs, high_refs = refs[0:3], refs[3:6], refs[6:9]
    norms = refs[9:11]
    outs, line = refs[11:14], refs[14]
    staged, lows, highs = refs[15], refs[16:19], refs[19:22]
    (load_sem, small_sem, send_sem, recv_sem, ready,
     train, change, norm_sem, chain_send, chain_recv) = refs[22:]
    me = lax.axis_index("shard")
    depth = staged.shape[1]
    counts = [weight.shape[1] // rows for weight in weights]
    starts = [sum(counts[:i]) for i in range(len(counts))]
    total = sum(counts)
    last = len(counts) - 1
    widths = [weight.shape[1] for weight in weights]
    plan = [cut(widths[0], [rows, 3 * rows]), cut(widths[1], []), last_pieces(widths[2])]
    pieces = [(which, i, *piece) for which in range(3) for i, piece in enumerate(plan[which])]

    def load(which, c):
        return pltpu.make_async_copy(
            weights[which].at[:, pl.ds(pl.multiple_of(c * rows, rows), rows)],
            staged.at[starts[which] + c],
            load_sem.at[starts[which] + c],
        )

    def low_copy(which):
        return pltpu.make_async_copy(low_refs[which], lows[which], small_sem.at[6 + which])

    def high_part(which, part):
        lo, hi = (0, rows) if part == 0 else (rows, highs[which].shape[1])
        here = (slice(None), pl.ds(lo, hi - lo))
        return pltpu.make_async_copy(
            high_refs[which].at[here], highs[which].at[here], small_sem.at[2 * which + part]
        )

    load(0, 0).start()
    low_copy(0).start()
    high_part(0, 0).start()

    barrier = pltpu.get_barrier_semaphore()

    @pl.when(me < n - 1)
    def _():
        pl.semaphore_signal(
            barrier, inc=1, device_id={"shard": jnp.minimum(me + 1, n - 1)},
            device_id_type=MESH,
        )

    @pl.when(me > 0)
    def _():
        pl.semaphore_wait(barrier, 1)
        pl.semaphore_signal(
            ready, inc=1, device_id={"shard": jnp.maximum(me - 1, 0)}, device_id_type=MESH
        )

    norm_loads = [
        pltpu.make_async_copy(norms[0], train, norm_sem.at[0]),
        pltpu.make_async_copy(norms[1], change, norm_sem.at[1]),
    ]

    def load_rest():
        for copy in norm_loads:
            copy.start()
        for which in range(3):
            if which:
                low_copy(which).start()
                high_part(which, 0).start()
            high_part(which, 1).start()

            @pl.loop(0 if which else 1, counts[which])
            def _(c):
                load(which, c).start()

    def block(p, owner):
        which, _, start, size = pieces[p]
        return outs[which].at[
            pl.ds(start, size), pl.ds(pl.multiple_of(owner * depth, 128), depth)
        ]

    def lane(step, way):
        return (0 if way > 0 else 1) * (n - 1) + step

    def ahead(way):
        return {"shard": jnp.clip(me + way, 0, n - 1)}

    def hop(p, step, way, owner):
        here = block(p, owner)
        slot = lane(step, way) * len(pieces) + p
        return pltpu.make_async_remote_copy(
            here, here, send_sem.at[slot], recv_sem.at[slot],
            device_id=ahead(way), device_id_type=MESH,
        )

    def chain(hops, way, owner):
        here = line.at[owner]
        return pltpu.make_async_remote_copy(
            here, here, chain_send.at[lane(hops, way)], chain_recv.at[lane(hops, way)],
            device_id=ahead(way), device_id_type=MESH,
        )

    def end(at, way):
        return at == (n - 1 if way > 0 else 0)

    def sends(step, way):
        owner = me - way * step
        ok = (owner >= 0) & (owner < n) & (me + way >= 0) & (me + way < n)
        return ok, jnp.clip(owner, 0, n - 1)

    def arrives(step, way):
        owner = me - way * (step + 1)
        return (owner >= 0) & (owner < n), jnp.clip(owner, 0, n - 1)

    def now(p, at, way):
        which, i = pieces[p][:2]
        if which != last:
            return True
        return jnp.logical_not(is_late(i, len(plan[last])) & end(at, way))

    def send(p, way):
        ok, owner = sends(0, way)
        ok = ok & now(p, me + way, way)
        pl.when(ok)(lambda: hop(p, 0, way, owner).start())

    def merge(which, c):
        load(which, c).wait()
        high = highs[which][:, pl.ds(pl.multiple_of(c * rows, rows), rows)]
        fresh = staged[starts[which] + c].T.astype(jnp.float32) + mix_rate * lax.dot_general(
            high, lows[which][...], (((0,), (0,)), ((), ())),
            preferred_element_type=jnp.float32,
        )
        outs[which][
            pl.ds(pl.multiple_of(c * rows, rows), rows),
            pl.ds(pl.multiple_of(me * depth, 128), depth),
        ] = fresh.astype(jnp.bfloat16)

    low_copy(0).wait()
    high_part(0, 0).wait()
    merge(0, 0)

    send(0, -1)
    pl.when(me < n - 1)(lambda: pl.semaphore_wait(ready, 1))
    send(0, 1)
    load_rest()
    for copy in norm_loads:
        copy.wait()
    line[me, 0, :] = train[...] + change[...]
    for way in (1, -1):
        ok, owner = sends(0, way)
        pl.when(ok)(lambda: chain(0, way, owner).start())
    for p, (which, i, start, size) in enumerate(pieces):
        if p == 0:
            continue
        if i == 0:
            low_copy(which).wait()
            high_part(which, 0).wait()
        if i == 0 or p == 1:
            high_part(which, 1).wait()
        pl.loop(pl.cdiv(start, rows), pl.cdiv(start + size, rows))(functools.partial(merge, which))
        send(p, -1)
        send(p, 1)

    def pass_norm(step):
        for way in (1, -1):
            ok, owner = arrives(step, way)
            further = ok & (me + way >= 0) & (me + way < n)
            pl.when(ok)(lambda: chain(step, way, owner).wait_recv())
            if step < n - 2:
                pl.when(further)(lambda: chain(step + 1, way, owner).start())

    def pass_on(p, step):
        for way in (1, -1):
            ok, owner = arrives(step, way)
            further = ok & (me + way >= 0) & (me + way < n) & now(p, me + way, way)
            ok = ok & now(p, me, way)
            pl.when(ok)(lambda: hop(p, step, way, owner).wait_recv())
            if step < n - 2:
                pl.when(further)(lambda: hop(p, step + 1, way, owner).start())

    for step in range(n - 1):
        pass_norm(step)
        for p in range(len(pieces)):
            pass_on(p, step)

    def sent(p, step):
        for way in (1, -1):
            ok, owner = sends(step, way)
            ok = ok & now(p, me + way, way)
            pl.when(ok)(lambda: hop(p, step, way, owner).wait_send())

    for step in range(n - 1):
        for way in (1, -1):
            ok, owner = sends(step, way)
            pl.when(ok)(lambda: chain(step, way, owner).wait_send())
        for p in range(len(pieces)):
            sent(p, step)


def gathered(n, rows, weights, lows, highs, train, step):
    depth = weights[0].shape[0]
    total = sum(weight.shape[1] // rows for weight in weights)
    vmem, hbm = pl.BlockSpec(memory_space=pltpu.VMEM), pl.BlockSpec(memory_space=pltpu.HBM)
    return pl.pallas_call(
        functools.partial(gather_kernel, n, rows),
        out_shape=[pltpu.VMEM((weight.shape[1], n * depth), jnp.bfloat16) for weight in weights]
        + [pltpu.VMEM((n, 1, train.shape[0]), jnp.float32)],
        in_specs=[hbm] * 11,
        out_specs=[vmem] * 4,
        scratch_shapes=[
            pltpu.VMEM((total, depth, rows), jnp.bfloat16),
            *[pltpu.VMEM(x.shape, x.dtype) for x in (*lows, *highs)],
            pltpu.SemaphoreType.DMA((total,)),
            pltpu.SemaphoreType.DMA((9,)),
            pltpu.SemaphoreType.DMA((2 * (n - 1) * total,)),
            pltpu.SemaphoreType.DMA((2 * (n - 1) * total,)),
            pltpu.SemaphoreType.REGULAR,
            pltpu.VMEM(train.shape, jnp.float32),
            pltpu.VMEM(step.shape, jnp.float32),
            pltpu.SemaphoreType.DMA((2,)),
            pltpu.SemaphoreType.DMA((2 * (n - 1),)),
            pltpu.SemaphoreType.DMA((2 * (n - 1),)),
        ],
        compiler_params=pltpu.CompilerParams(
            collective_id=0, has_side_effects=True, vmem_limit_bytes=47 * 2**20
        ),
        name="gather",
    )(*weights, *lows, *highs, train, step)


def flush_kernel(n, count, *refs):
    sources, held = refs[:count], refs[count]
    results, result = refs[count + 1 : 2 * count + 1], refs[2 * count + 1]
    token, sems, held_sems = refs[2 * count + 2 :]
    me = lax.axis_index("shard")
    depth = held.shape[1] // n
    pieces = last_pieces(held.shape[0])
    outer = (me == 0) | (me == n - 1)

    def each(act):
        for i, (source, to) in enumerate(zip(sources, results)):
            act(pltpu.make_async_copy(source, to, sems.at[i]))
        for i, (start, size) in enumerate(pieces):
            rows = pl.ds(start, size)
            late = outer & is_late(i, len(pieces))

            @pl.when(jnp.logical_not(late))
            def _():
                act(pltpu.make_async_copy(
                    held.at[rows, :], result.at[rows, :], held_sems.at[i]
                ))

            @pl.when(late)
            def _():
                here = (rows, pl.ds(pl.multiple_of(me * depth, 128), depth))
                act(pltpu.make_async_copy(held.at[here], result.at[here], held_sems.at[i]))

    each(lambda copy: copy.start())
    token[...] = jnp.zeros_like(token)
    each(lambda copy: copy.wait())


def flushed(n, done, held):
    vmem, hbm = pl.BlockSpec(memory_space=pltpu.VMEM), pl.BlockSpec(memory_space=pltpu.HBM)
    return pl.pallas_call(
        functools.partial(flush_kernel, n, len(done)),
        out_shape=[jax.ShapeDtypeStruct(x.shape, x.dtype) for x in (*done, held)]
        + [pltpu.VMEM((8, 128), jnp.float32)],
        in_specs=[vmem] * (len(done) + 1),
        out_specs=[hbm] * (len(done) + 1) + [vmem],
        scratch_shapes=[
            pltpu.SemaphoreType.DMA((len(done),)),
            pltpu.SemaphoreType.DMA((len(last_pieces(held.shape[0])),)),
        ],
        compiler_params=pltpu.CompilerParams(vmem_limit_bytes=2**20),
        name="flush",
    )(*done, held)


def lay_out(parts, flat):
    tp, n, _, part = parts.shape
    for row in range(flat.shape[0]):
        cells, at = [], row * 128
        while at < (row + 1) * 128:
            slot, lo = divmod(at, part)
            size = min(part - lo, (row + 1) * 128 - at)
            cells.append(parts[slot % tp, slot // tp, 0:1, lo : lo + size])
            at += size
        flat[row : row + 1, :] = jnp.concatenate(cells, axis=1) if len(cells) > 1 else cells[0]


def tail_kernel(n, tp, depth, held, line, token, tail, norm_out, *scratch):
    lines, norm_flat, send_sem, recv_sem, side_send, side_recv = scratch
    me, my_tp = lax.axis_index("shard"), lax.axis_index("tp")
    pieces = last_pieces(held.shape[0])
    ends = ((1, n - 1), (-1, 0))

    core = lax.rem(lax.axis_index("trial"), 2)
    pl.when((core == 1) & ((me == 0) | (me == n - 1)))(lambda: pl.delay(YIELD_NS))

    barrier = pltpu.get_barrier_semaphore()
    for way, at in ends:
        @pl.when(me == at)
        def _():
            pl.semaphore_signal(
                barrier, inc=1, device_id={"shard": at - way}, device_id_type=MESH
            )
    for t in range(1, tp):
        pl.semaphore_signal(
            barrier, inc=1, device_id={"tp": lax.rem(my_tp + t, tp)}, device_id_type=MESH
        )
    lines[my_tp] = line[...]
    greeted = sum(jnp.where(me == at - way, 1, 0) for way, at in ends) + tp - 1
    pl.when(greeted > 0)(lambda: pl.semaphore_wait(barrier, greeted))

    def each(way, at, away, act):
        for i, (start, size) in enumerate(pieces):
            here = (pl.ds(start, size), pl.ds(0 if way > 0 else depth, (n - 1) * depth))
            slot = (0 if way > 0 else len(pieces)) + i

            @pl.when((me == at - away) & is_late(i, len(pieces)))
            def _():
                act(pltpu.make_async_remote_copy(
                    held.at[here], tail.at[here], send_sem.at[slot], recv_sem.at[slot],
                    device_id={"shard": at}, device_id_type=MESH,
                ))

    def side(t, column):
        return pltpu.make_async_remote_copy(
            line, lines.at[column], side_send.at[t - 1], side_recv.at[t - 1],
            device_id={"tp": lax.rem(my_tp + t, tp)}, device_id_type=MESH,
        )

    for way, at in ends:
        each(way, at, way, lambda copy: copy.start())
    for t in range(1, tp):
        side(t, my_tp).start()
    for t in range(1, tp):
        side(t, lax.rem(my_tp - t + tp, tp)).wait_recv()
    lay_out(lines, norm_flat)
    norm_out[...] = norm_flat[...].astype(jnp.bfloat16)
    for way, at in ends:
        each(way, at, 0, lambda copy: copy.wait_recv())
    for way, at in ends:
        each(way, at, way, lambda copy: copy.wait_send())
    for t in range(1, tp):
        side(t, my_tp).wait_send()


def tailed(n, tp, depth, held, line, token):
    vmem = pl.BlockSpec(memory_space=pltpu.VMEM)
    count = len(last_pieces(held.shape[0]))
    lines = (tp, *line.shape)
    flat = (math.prod(lines) // 128, 128)
    return pl.pallas_call(
        functools.partial(tail_kernel, n, tp, depth),
        out_shape=[pltpu.VMEM(held.shape, held.dtype), pltpu.VMEM(flat, jnp.bfloat16)],
        in_specs=[vmem] * 3,
        out_specs=[vmem] * 2,
        scratch_shapes=[
            pltpu.VMEM(lines, jnp.float32),
            pltpu.VMEM(flat, jnp.float32),
            pltpu.SemaphoreType.DMA((2 * count,)),
            pltpu.SemaphoreType.DMA((2 * count,)),
            pltpu.SemaphoreType.DMA((max(tp - 1, 1),)),
            pltpu.SemaphoreType.DMA((max(tp - 1, 1),)),
        ],
        compiler_params=pltpu.CompilerParams(
            collective_id=1, has_side_effects=True, vmem_limit_bytes=2**20
        ),
        name="tail",
    )(held, line, token)


def close_kernel(n, tail, norm, begun, result, norm_out, sems):
    me = lax.axis_index("shard")
    pieces = last_pieces(tail.shape[0])
    depth = tail.shape[1] // n

    def each(act):
        for at in (0, n - 1):
            for i, (start, size) in enumerate(pieces):
                here = (pl.ds(start, size), pl.ds(0 if at else depth, (n - 1) * depth))

                @pl.when((me == at) & is_late(i, len(pieces)))
                def _():
                    act(pltpu.make_async_copy(tail.at[here], result.at[here], sems.at[i]))
        act(pltpu.make_async_copy(norm, norm_out, sems.at[len(pieces)]))

    each(lambda copy: copy.start())
    each(lambda copy: copy.wait())


def closed(n, tail, norm, begun):
    vmem, hbm = pl.BlockSpec(memory_space=pltpu.VMEM), pl.BlockSpec(memory_space=pltpu.HBM)
    return pl.pallas_call(
        functools.partial(close_kernel, n),
        out_shape=[jax.ShapeDtypeStruct(x.shape, x.dtype) for x in (begun, norm)],
        in_specs=[vmem, vmem, hbm],
        out_specs=[hbm] * 2,
        input_output_aliases={2: 0},
        scratch_shapes=[pltpu.SemaphoreType.DMA((len(last_pieces(tail.shape[0])) + 1,))],
        compiler_params=pltpu.CompilerParams(vmem_limit_bytes=2**20),
        name="close",
    )(tail, norm, begun)


def plain(weights, lows, highs, norm_new):
    serve = []
    for weight, low, high in zip(weights, lows, highs):
        fresh = weight.astype(jnp.float32) + mix_rate * jnp.dot(
            low, high, preferred_element_type=jnp.float32
        )
        serve.append(
            lax.all_gather(fresh.astype(jnp.bfloat16), "shard", axis=0, tiled=True).T
        )
    norm = lax.all_gather(
        norm_new.astype(jnp.bfloat16), ("shard", "tp"), axis=0, tiled=True
    )
    return (*serve, norm)


def on_device(n, tp, wq, lq, hq, wk, lk, hk, wv, lv, hv, norm_train, norm_step):
    weights, lows, highs = (wq, wk, wv), (lq, lk, lv), (hq, hk, hv)
    depth = wq.shape[0]
    if n < 2 or depth % 128 or any(w.shape[1] % ROWS or w.shape[1] < 2 * ROWS for w in weights):
        return plain(weights, lows, highs, norm_train + norm_step)
    query, key, value, line = gathered(
        n, ROWS, weights, [low.T for low in lows], highs, norm_train, norm_step
    )
    query, key, begun, token = flushed(n, [query, key], value)
    tail, norm = tailed(n, tp, depth, value, line, token)
    value, norm = closed(n, tail, norm, begun)
    return (query, key, value, norm.reshape(-1))


def solution(mesh):
    in_specs = (
        (P(("trial", "shard"), "tp"), P(("trial", "shard"), None), P("trial", "tp")) * 3
        + (P(("trial", "shard", "tp")),) * 2
    )
    out_specs = (P(("trial", "tp"), None),) * 3 + (P("trial"),)
    body = functools.partial(on_device, mesh.shape["shard"], mesh.shape["tp"])
    return jax.shard_map(
        body, mesh=mesh, in_specs=in_specs, out_specs=out_specs, check_vma=False
    )
```

```python
import functools
import math

import jax
import jax.numpy as jnp
from jax import lax
from jax.experimental import pallas as pl
from jax.experimental.pallas import tpu as pltpu
from jax.sharding import PartitionSpec as P

mix_rate = 1.0
MESH = pl.DeviceIdType.MESH
ROWS = 128
PIECE = 2048
LATE = (2, 1)
YIELD_NS = 4000


def cut(width, sizes):
    pieces, at = [], 0
    while at < width:
        size = min(sizes[len(pieces)] if len(pieces) < len(sizes) else PIECE, width - at)
        pieces.append((at, size))
        at += size
    return pieces


def last_pieces(width):
    return cut(width, [width - ROWS, ROWS])


def is_late(index, count):
    core = lax.rem(lax.axis_index("trial"), 2)
    late = [index >= count - x for x in LATE]
    if late[0] == late[1]:
        return late[0]
    return core == (0 if late[0] else 1)


def gather_kernel(n, rows, *refs):
    weights, low_refs, high_refs = refs[0:3], refs[3:6], refs[6:9]
    norms = refs[9:11]
    outs, line = refs[11:14], refs[14]
    staged, lows, highs = refs[15], refs[16:19], refs[19:22]
    (load_sem, small_sem, send_sem, recv_sem, ready,
     train, change, norm_sem, chain_send, chain_recv) = refs[22:]
    me = lax.axis_index("shard")
    depth = staged.shape[1]
    counts = [weight.shape[1] // rows for weight in weights]
    starts = [sum(counts[:i]) for i in range(len(counts))]
    total = sum(counts)
    last = len(counts) - 1
    widths = [weight.shape[1] for weight in weights]
    plan = [cut(widths[0], [rows, 3 * rows]), cut(widths[1], []), last_pieces(widths[2])]
    pieces = [(which, i, *piece) for which in range(3) for i, piece in enumerate(plan[which])]

    def load(which, c):
        return pltpu.make_async_copy(
            weights[which].at[:, pl.ds(pl.multiple_of(c * rows, rows), rows)],
            staged.at[starts[which] + c],
            load_sem.at[starts[which] + c],
        )

    def low_copy(which):
        return pltpu.make_async_copy(low_refs[which], lows[which], small_sem.at[6 + which])

    def high_part(which, part):
        lo, hi = (0, rows) if part == 0 else (rows, highs[which].shape[1])
        here = (slice(None), pl.ds(lo, hi - lo))
        return pltpu.make_async_copy(
            high_refs[which].at[here], highs[which].at[here], small_sem.at[2 * which + part]
        )

    low_copy(0).start(priority=1)
    high_part(0, 0).start(priority=1)
    load(0, 0).start()

    barrier = pltpu.get_barrier_semaphore()

    @pl.when(me < n - 1)
    def _():
        pl.semaphore_signal(
            barrier, inc=1, device_id={"shard": jnp.minimum(me + 1, n - 1)},
            device_id_type=MESH,
        )

    @pl.when(me > 0)
    def _():
        pl.semaphore_wait(barrier, 1)
        pl.semaphore_signal(
            ready, inc=1, device_id={"shard": jnp.maximum(me - 1, 0)}, device_id_type=MESH
        )

    norm_loads = [
        pltpu.make_async_copy(norms[0], train, norm_sem.at[0]),
        pltpu.make_async_copy(norms[1], change, norm_sem.at[1]),
    ]

    def load_rest():
        for copy in norm_loads:
            copy.start()
        for which in range(3):
            if which:
                low_copy(which).start()
                high_part(which, 0).start()
            high_part(which, 1).start()

            @pl.loop(0 if which else 1, counts[which])
            def _(c):
                load(which, c).start()

    def block(p, owner):
        which, _, start, size = pieces[p]
        return outs[which].at[
            pl.ds(start, size), pl.ds(pl.multiple_of(owner * depth, 128), depth)
        ]

    def lane(step, way):
        return (0 if way > 0 else 1) * (n - 1) + step

    def ahead(way):
        return {"shard": jnp.clip(me + way, 0, n - 1)}

    def hop(p, step, way, owner):
        here = block(p, owner)
        slot = lane(step, way) * len(pieces) + p
        return pltpu.make_async_remote_copy(
            here, here, send_sem.at[slot], recv_sem.at[slot],
            device_id=ahead(way), device_id_type=MESH,
        )

    def chain(hops, way, owner):
        here = line.at[owner]
        return pltpu.make_async_remote_copy(
            here, here, chain_send.at[lane(hops, way)], chain_recv.at[lane(hops, way)],
            device_id=ahead(way), device_id_type=MESH,
        )

    def end(at, way):
        return at == (n - 1 if way > 0 else 0)

    def sends(step, way):
        owner = me - way * step
        ok = (owner >= 0) & (owner < n) & (me + way >= 0) & (me + way < n)
        return ok, jnp.clip(owner, 0, n - 1)

    def arrives(step, way):
        owner = me - way * (step + 1)
        return (owner >= 0) & (owner < n), jnp.clip(owner, 0, n - 1)

    def now(p, at, way):
        which, i = pieces[p][:2]
        if which != last:
            return True
        return jnp.logical_not(is_late(i, len(plan[last])) & end(at, way))

    def send(p, way):
        ok, owner = sends(0, way)
        ok = ok & now(p, me + way, way)
        pl.when(ok)(lambda: hop(p, 0, way, owner).start())

    def merge(which, c):
        load(which, c).wait()
        high = highs[which][:, pl.ds(pl.multiple_of(c * rows, rows), rows)]
        fresh = staged[starts[which] + c].T.astype(jnp.float32) + mix_rate * lax.dot_general(
            high, lows[which][...], (((0,), (0,)), ((), ())),
            preferred_element_type=jnp.float32,
        )
        outs[which][
            pl.ds(pl.multiple_of(c * rows, rows), rows),
            pl.ds(pl.multiple_of(me * depth, 128), depth),
        ] = fresh.astype(jnp.bfloat16)

    low_copy(0).wait()
    high_part(0, 0).wait()
    merge(0, 0)

    send(0, -1)
    pl.when(me < n - 1)(lambda: pl.semaphore_wait(ready, 1))
    send(0, 1)
    load_rest()
    for copy in norm_loads:
        copy.wait()
    line[me, 0, :] = train[...] + change[...]
    for way in (1, -1):
        ok, owner = sends(0, way)
        pl.when(ok)(lambda: chain(0, way, owner).start())
    for p, (which, i, start, size) in enumerate(pieces):
        if p == 0:
            continue
        if i == 0:
            low_copy(which).wait()
            high_part(which, 0).wait()
        if i == 0 or p == 1:
            high_part(which, 1).wait()
        pl.loop(start // rows, (start + size) // rows)(functools.partial(merge, which))
        send(p, -1)
        send(p, 1)

    def pass_norm(step):
        for way in (1, -1):
            ok, owner = arrives(step, way)
            further = ok & (me + way >= 0) & (me + way < n)
            pl.when(ok)(lambda: chain(step, way, owner).wait_recv())
            if step < n - 2:
                pl.when(further)(lambda: chain(step + 1, way, owner).start())

    def pass_on(p, step):
        for way in (1, -1):
            ok, owner = arrives(step, way)
            further = ok & (me + way >= 0) & (me + way < n) & now(p, me + way, way)
            ok = ok & now(p, me, way)
            pl.when(ok)(lambda: hop(p, step, way, owner).wait_recv())
            if step < n - 2:
                pl.when(further)(lambda: hop(p, step + 1, way, owner).start())

    for step in range(n - 1):
        pass_norm(step)
        for p in range(len(pieces)):
            pass_on(p, step)

    def sent(p, step):
        for way in (1, -1):
            ok, owner = sends(step, way)
            ok = ok & now(p, me + way, way)
            pl.when(ok)(lambda: hop(p, step, way, owner).wait_send())

    for step in range(n - 1):
        for way in (1, -1):
            ok, owner = sends(step, way)
            pl.when(ok)(lambda: chain(step, way, owner).wait_send())
        for p in range(len(pieces)):
            sent(p, step)


def gathered(n, rows, weights, lows, highs, train, step):
    depth = weights[0].shape[0]
    total = sum(weight.shape[1] // rows for weight in weights)
    vmem, hbm = pl.BlockSpec(memory_space=pltpu.VMEM), pl.BlockSpec(memory_space=pltpu.HBM)
    return pl.pallas_call(
        functools.partial(gather_kernel, n, rows),
        out_shape=[pltpu.VMEM((weight.shape[1], n * depth), jnp.bfloat16) for weight in weights]
        + [pltpu.VMEM((n, 1, train.shape[0]), jnp.float32)],
        in_specs=[hbm] * 11,
        out_specs=[vmem] * 4,
        scratch_shapes=[
            pltpu.VMEM((total, depth, rows), jnp.bfloat16),
            *[pltpu.VMEM(x.shape, x.dtype) for x in (*lows, *highs)],
            pltpu.SemaphoreType.DMA((total,)),
            pltpu.SemaphoreType.DMA((9,)),
            pltpu.SemaphoreType.DMA((2 * (n - 1) * total,)),
            pltpu.SemaphoreType.DMA((2 * (n - 1) * total,)),
            pltpu.SemaphoreType.REGULAR,
            pltpu.VMEM(train.shape, jnp.float32),
            pltpu.VMEM(step.shape, jnp.float32),
            pltpu.SemaphoreType.DMA((2,)),
            pltpu.SemaphoreType.DMA((2 * (n - 1),)),
            pltpu.SemaphoreType.DMA((2 * (n - 1),)),
        ],
        compiler_params=pltpu.CompilerParams(
            collective_id=0, has_side_effects=True, vmem_limit_bytes=47 * 2**20
        ),
        name="gather",
    )(*weights, *lows, *highs, train, step)


def flush_kernel(n, count, *refs):
    sources, held = refs[:count], refs[count]
    results, result = refs[count + 1 : 2 * count + 1], refs[2 * count + 1]
    token, sems, held_sems = refs[2 * count + 2 :]
    me = lax.axis_index("shard")
    depth = held.shape[1] // n
    pieces = last_pieces(held.shape[0])
    outer = (me == 0) | (me == n - 1)

    def each(act):
        for i, (source, to) in enumerate(zip(sources, results)):
            act(pltpu.make_async_copy(source, to, sems.at[i]))
        for i, (start, size) in enumerate(pieces):
            rows = pl.ds(start, size)
            late = outer & is_late(i, len(pieces))

            @pl.when(jnp.logical_not(late))
            def _():
                act(pltpu.make_async_copy(
                    held.at[rows, :], result.at[rows, :], held_sems.at[i]
                ))

            @pl.when(late)
            def _():
                here = (rows, pl.ds(pl.multiple_of(me * depth, 128), depth))
                act(pltpu.make_async_copy(held.at[here], result.at[here], held_sems.at[i]))

    each(lambda copy: copy.start())
    token[...] = jnp.zeros_like(token)
    each(lambda copy: copy.wait())


def flushed(n, done, held):
    vmem, hbm = pl.BlockSpec(memory_space=pltpu.VMEM), pl.BlockSpec(memory_space=pltpu.HBM)
    return pl.pallas_call(
        functools.partial(flush_kernel, n, len(done)),
        out_shape=[jax.ShapeDtypeStruct(x.shape, x.dtype) for x in (*done, held)]
        + [pltpu.VMEM((8, 128), jnp.float32)],
        in_specs=[vmem] * (len(done) + 1),
        out_specs=[hbm] * (len(done) + 1) + [vmem],
        scratch_shapes=[
            pltpu.SemaphoreType.DMA((len(done),)),
            pltpu.SemaphoreType.DMA((len(last_pieces(held.shape[0])),)),
        ],
        compiler_params=pltpu.CompilerParams(vmem_limit_bytes=2**20),
        name="flush",
    )(*done, held)


def lay_out(parts, flat):
    tp, n, _, part = parts.shape
    for row in range(flat.shape[0]):
        cells, at = [], row * 128
        while at < (row + 1) * 128:
            slot, lo = divmod(at, part)
            size = min(part - lo, (row + 1) * 128 - at)
            cells.append(parts[slot % tp, slot // tp, 0:1, lo : lo + size])
            at += size
        flat[row : row + 1, :] = jnp.concatenate(cells, axis=1) if len(cells) > 1 else cells[0]


def tail_kernel(n, tp, depth, held, line, token, tail, norm_out, *scratch):
    lines, norm_flat, send_sem, recv_sem, side_send, side_recv = scratch
    me, my_tp = lax.axis_index("shard"), lax.axis_index("tp")
    pieces = last_pieces(held.shape[0])
    ends = ((1, n - 1), (-1, 0))

    core = lax.rem(lax.axis_index("trial"), 2)
    pl.when((core == 1) & ((me == 0) | (me == n - 1)))(lambda: pl.delay(YIELD_NS))

    barrier = pltpu.get_barrier_semaphore()
    for way, at in ends:
        @pl.when(me == at)
        def _():
            pl.semaphore_signal(
                barrier, inc=1, device_id={"shard": at - way}, device_id_type=MESH
            )
    for t in range(1, tp):
        pl.semaphore_signal(
            barrier, inc=1, device_id={"tp": lax.rem(my_tp + t, tp)}, device_id_type=MESH
        )
    lines[my_tp] = line[...]
    greeted = sum(jnp.where(me == at - way, 1, 0) for way, at in ends) + tp - 1
    pl.when(greeted > 0)(lambda: pl.semaphore_wait(barrier, greeted))

    def each(way, at, away, act):
        for i, (start, size) in enumerate(pieces):
            here = (pl.ds(start, size), pl.ds(0 if way > 0 else depth, (n - 1) * depth))
            slot = (0 if way > 0 else len(pieces)) + i

            @pl.when((me == at - away) & is_late(i, len(pieces)))
            def _():
                act(pltpu.make_async_remote_copy(
                    held.at[here], tail.at[here], send_sem.at[slot], recv_sem.at[slot],
                    device_id={"shard": at}, device_id_type=MESH,
                ))

    def side(t, column):
        return pltpu.make_async_remote_copy(
            line, lines.at[column], side_send.at[t - 1], side_recv.at[t - 1],
            device_id={"tp": lax.rem(my_tp + t, tp)}, device_id_type=MESH,
        )

    for way, at in ends:
        each(way, at, way, lambda copy: copy.start())
    for t in range(1, tp):
        side(t, my_tp).start()
    for t in range(1, tp):
        side(t, lax.rem(my_tp - t + tp, tp)).wait_recv()
    lay_out(lines, norm_flat)
    norm_out[...] = norm_flat[...].astype(jnp.bfloat16)
    for way, at in ends:
        each(way, at, 0, lambda copy: copy.wait_recv())
    for way, at in ends:
        each(way, at, way, lambda copy: copy.wait_send())
    for t in range(1, tp):
        side(t, my_tp).wait_send()


def tailed(n, tp, depth, held, line, token):
    vmem = pl.BlockSpec(memory_space=pltpu.VMEM)
    count = len(last_pieces(held.shape[0]))
    lines = (tp, *line.shape)
    flat = (math.prod(lines) // 128, 128)
    return pl.pallas_call(
        functools.partial(tail_kernel, n, tp, depth),
        out_shape=[pltpu.VMEM(held.shape, held.dtype), pltpu.VMEM(flat, jnp.bfloat16)],
        in_specs=[vmem] * 3,
        out_specs=[vmem] * 2,
        scratch_shapes=[
            pltpu.VMEM(lines, jnp.float32),
            pltpu.VMEM(flat, jnp.float32),
            pltpu.SemaphoreType.DMA((2 * count,)),
            pltpu.SemaphoreType.DMA((2 * count,)),
            pltpu.SemaphoreType.DMA((max(tp - 1, 1),)),
            pltpu.SemaphoreType.DMA((max(tp - 1, 1),)),
        ],
        compiler_params=pltpu.CompilerParams(
            collective_id=1, has_side_effects=True, vmem_limit_bytes=2**20
        ),
        name="tail",
    )(held, line, token)


def close_kernel(n, tail, norm, begun, result, norm_out, sems):
    me = lax.axis_index("shard")
    pieces = last_pieces(tail.shape[0])
    depth = tail.shape[1] // n

    def each(act):
        for at in (0, n - 1):
            for i, (start, size) in enumerate(pieces):
                here = (pl.ds(start, size), pl.ds(0 if at else depth, (n - 1) * depth))

                @pl.when((me == at) & is_late(i, len(pieces)))
                def _():
                    act(pltpu.make_async_copy(tail.at[here], result.at[here], sems.at[i]))
        act(pltpu.make_async_copy(norm, norm_out, sems.at[len(pieces)]))

    each(lambda copy: copy.start())
    each(lambda copy: copy.wait())


def closed(n, tail, norm, begun):
    vmem, hbm = pl.BlockSpec(memory_space=pltpu.VMEM), pl.BlockSpec(memory_space=pltpu.HBM)
    return pl.pallas_call(
        functools.partial(close_kernel, n),
        out_shape=[jax.ShapeDtypeStruct(x.shape, x.dtype) for x in (begun, norm)],
        in_specs=[vmem, vmem, hbm],
        out_specs=[hbm] * 2,
        input_output_aliases={2: 0},
        scratch_shapes=[pltpu.SemaphoreType.DMA((len(last_pieces(tail.shape[0])) + 1,))],
        compiler_params=pltpu.CompilerParams(vmem_limit_bytes=2**20),
        name="close",
    )(tail, norm, begun)


def plain(weights, lows, highs, norm_new):
    serve = []
    for weight, low, high in zip(weights, lows, highs):
        fresh = weight.astype(jnp.float32) + mix_rate * jnp.dot(
            low, high, preferred_element_type=jnp.float32
        )
        serve.append(
            lax.all_gather(fresh.astype(jnp.bfloat16), "shard", axis=0, tiled=True).T
        )
    norm = lax.all_gather(
        norm_new.astype(jnp.bfloat16), ("shard", "tp"), axis=0, tiled=True
    )
    return (*serve, norm)


def on_device(n, tp, wq, lq, hq, wk, lk, hk, wv, lv, hv, norm_train, norm_step):
    weights, lows, highs = (wq, wk, wv), (lq, lk, lv), (hq, hk, hv)
    depth = wq.shape[0]
    if n < 2 or depth % 128 or any(w.shape[1] % ROWS or w.shape[1] < 2 * ROWS for w in weights):
        return plain(weights, lows, highs, norm_train + norm_step)
    query, key, value, line = gathered(
        n, ROWS, weights, [low.T for low in lows], highs, norm_train, norm_step
    )
    query, key, begun, token = flushed(n, [query, key], value)
    tail, norm = tailed(n, tp, depth, value, line, token)
    value, norm = closed(n, tail, norm, begun)
    return (query, key, value, norm.reshape(-1))


def solution(mesh):
    in_specs = (
        (P(("trial", "shard"), "tp"), P(("trial", "shard"), None), P("trial", "tp")) * 3
        + (P(("trial", "shard", "tp")),) * 2
    )
    out_specs = (P(("trial", "tp"), None),) * 3 + (P("trial"),)
    body = functools.partial(on_device, mesh.shape["shard"], mesh.shape["tp"])
    return jax.shard_map(
        body, mesh=mesh, in_specs=in_specs, out_specs=out_specs, check_vma=False
    )
```

```python
import functools
import math

import jax
import jax.numpy as jnp
from jax import lax
from jax.experimental import pallas as pl
from jax.experimental.pallas import tpu as pltpu
from jax.sharding import PartitionSpec as P

mix_rate = 1.0
MESH = pl.DeviceIdType.MESH
ROWS = 128
PIECE = 1024
LATE = (2, 1)
YIELD_NS = 4000


def cut(width, sizes):
    pieces, at = [], 0
    while at < width:
        size = min(sizes[len(pieces)] if len(pieces) < len(sizes) else PIECE, width - at)
        pieces.append((at, size))
        at += size
    return pieces


def last_pieces(width):
    return cut(width, [width - ROWS, ROWS])


def is_late(index, count):
    core = lax.rem(lax.axis_index("trial"), 2)
    late = [index >= count - x for x in LATE]
    if late[0] == late[1]:
        return late[0]
    return core == (0 if late[0] else 1)


def gather_kernel(n, rows, *refs):
    weights, low_refs, high_refs = refs[0:3], refs[3:6], refs[6:9]
    norms = refs[9:11]
    outs, line = refs[11:14], refs[14]
    staged, lows, highs = refs[15], refs[16:19], refs[19:22]
    (load_sem, small_sem, send_sem, recv_sem, ready,
     train, change, norm_sem, chain_send, chain_recv) = refs[22:]
    me = lax.axis_index("shard")
    depth = staged.shape[1]
    counts = [weight.shape[1] // rows for weight in weights]
    starts = [sum(counts[:i]) for i in range(len(counts))]
    total = sum(counts)
    last = len(counts) - 1
    widths = [weight.shape[1] for weight in weights]
    plan = [cut(widths[0], [rows, 3 * rows]), cut(widths[1], []), last_pieces(widths[2])]
    pieces = [(which, i, *piece) for which in range(3) for i, piece in enumerate(plan[which])]

    def load(which, c):
        return pltpu.make_async_copy(
            weights[which].at[:, pl.ds(pl.multiple_of(c * rows, rows), rows)],
            staged.at[starts[which] + c],
            load_sem.at[starts[which] + c],
        )

    def low_copy(which):
        return pltpu.make_async_copy(low_refs[which], lows[which], small_sem.at[6 + which])

    def high_part(which, part):
        lo, hi = (0, rows) if part == 0 else (rows, highs[which].shape[1])
        here = (slice(None), pl.ds(lo, hi - lo))
        return pltpu.make_async_copy(
            high_refs[which].at[here], highs[which].at[here], small_sem.at[2 * which + part]
        )

    load(0, 0).start()
    low_copy(0).start()
    high_part(0, 0).start()

    barrier = pltpu.get_barrier_semaphore()

    @pl.when(me < n - 1)
    def _():
        pl.semaphore_signal(
            barrier, inc=1, device_id={"shard": jnp.minimum(me + 1, n - 1)},
            device_id_type=MESH,
        )

    @pl.when(me > 0)
    def _():
        pl.semaphore_wait(barrier, 1)
        pl.semaphore_signal(
            ready, inc=1, device_id={"shard": jnp.maximum(me - 1, 0)}, device_id_type=MESH
        )

    norm_loads = [
        pltpu.make_async_copy(norms[0], train, norm_sem.at[0]),
        pltpu.make_async_copy(norms[1], change, norm_sem.at[1]),
    ]

    def load_rest():
        for copy in norm_loads:
            copy.start()
        for which in range(3):
            if which:
                low_copy(which).start()
                high_part(which, 0).start()
            high_part(which, 1).start()

            @pl.loop(0 if which else 1, counts[which])
            def _(c):
                load(which, c).start()

    def block(p, owner):
        which, _, start, size = pieces[p]
        return outs[which].at[
            pl.ds(start, size), pl.ds(pl.multiple_of(owner * depth, 128), depth)
        ]

    def lane(step, way):
        return (0 if way > 0 else 1) * (n - 1) + step

    def ahead(way):
        return {"shard": jnp.clip(me + way, 0, n - 1)}

    def hop(p, step, way, owner):
        here = block(p, owner)
        slot = lane(step, way) * len(pieces) + p
        return pltpu.make_async_remote_copy(
            here, here, send_sem.at[slot], recv_sem.at[slot],
            device_id=ahead(way), device_id_type=MESH,
        )

    def chain(hops, way, owner):
        here = line.at[owner]
        return pltpu.make_async_remote_copy(
            here, here, chain_send.at[lane(hops, way)], chain_recv.at[lane(hops, way)],
            device_id=ahead(way), device_id_type=MESH,
        )

    def end(at, way):
        return at == (n - 1 if way > 0 else 0)

    def sends(step, way):
        owner = me - way * step
        ok = (owner >= 0) & (owner < n) & (me + way >= 0) & (me + way < n)
        return ok, jnp.clip(owner, 0, n - 1)

    def arrives(step, way):
        owner = me - way * (step + 1)
        return (owner >= 0) & (owner < n), jnp.clip(owner, 0, n - 1)

    def now(p, at, way):
        which, i = pieces[p][:2]
        if which != last:
            return True
        return jnp.logical_not(is_late(i, len(plan[last])) & end(at, way))

    def send(p, way):
        ok, owner = sends(0, way)
        ok = ok & now(p, me + way, way)
        pl.when(ok)(lambda: hop(p, 0, way, owner).start())

    def merge(which, c):
        load(which, c).wait()
        high = highs[which][:, pl.ds(pl.multiple_of(c * rows, rows), rows)]
        fresh = staged[starts[which] + c].T.astype(jnp.float32) + mix_rate * lax.dot_general(
            high, lows[which][...], (((0,), (0,)), ((), ())),
            preferred_element_type=jnp.float32,
        )
        outs[which][
            pl.ds(pl.multiple_of(c * rows, rows), rows),
            pl.ds(pl.multiple_of(me * depth, 128), depth),
        ] = fresh.astype(jnp.bfloat16)

    low_copy(0).wait()
    high_part(0, 0).wait()
    merge(0, 0)

    send(0, -1)
    pl.when(me < n - 1)(lambda: pl.semaphore_wait(ready, 1))
    send(0, 1)
    load_rest()

    def start_norm():
        for copy in norm_loads:
            copy.wait()
        line[me, 0, :] = train[...] + change[...]
        for way in (1, -1):
            ok, owner = sends(0, way)
            pl.when(ok)(lambda: chain(0, way, owner).start())

    for p, (which, i, start, size) in enumerate(pieces):
        if p == 0:
            continue
        if i == 0:
            low_copy(which).wait()
            high_part(which, 0).wait()
        if i == 0 or p == 1:
            high_part(which, 1).wait()
        pl.loop(start // rows, (start + size) // rows)(functools.partial(merge, which))
        send(p, -1)
        send(p, 1)
        if p == 1:
            start_norm()

    def pass_norm(step):
        for way in (1, -1):
            ok, owner = arrives(step, way)
            further = ok & (me + way >= 0) & (me + way < n)
            pl.when(ok)(lambda: chain(step, way, owner).wait_recv())
            if step < n - 2:
                pl.when(further)(lambda: chain(step + 1, way, owner).start())

    def pass_on(p, step):
        for way in (1, -1):
            ok, owner = arrives(step, way)
            further = ok & (me + way >= 0) & (me + way < n) & now(p, me + way, way)
            ok = ok & now(p, me, way)
            pl.when(ok)(lambda: hop(p, step, way, owner).wait_recv())
            if step < n - 2:
                pl.when(further)(lambda: hop(p, step + 1, way, owner).start())

    for step in range(n - 1):
        pass_norm(step)
        for p in range(len(pieces)):
            pass_on(p, step)

    def sent(p, step):
        for way in (1, -1):
            ok, owner = sends(step, way)
            ok = ok & now(p, me + way, way)
            pl.when(ok)(lambda: hop(p, step, way, owner).wait_send())

    for step in range(n - 1):
        for way in (1, -1):
            ok, owner = sends(step, way)
            pl.when(ok)(lambda: chain(step, way, owner).wait_send())
        for p in range(len(pieces)):
            sent(p, step)


def gathered(n, rows, weights, lows, highs, train, step):
    depth = weights[0].shape[0]
    total = sum(weight.shape[1] // rows for weight in weights)
    vmem, hbm = pl.BlockSpec(memory_space=pltpu.VMEM), pl.BlockSpec(memory_space=pltpu.HBM)
    return pl.pallas_call(
        functools.partial(gather_kernel, n, rows),
        out_shape=[pltpu.VMEM((weight.shape[1], n * depth), jnp.bfloat16) for weight in weights]
        + [pltpu.VMEM((n, 1, train.shape[0]), jnp.float32)],
        in_specs=[hbm] * 11,
        out_specs=[vmem] * 4,
        scratch_shapes=[
            pltpu.VMEM((total, depth, rows), jnp.bfloat16),
            *[pltpu.VMEM(x.shape, x.dtype) for x in (*lows, *highs)],
            pltpu.SemaphoreType.DMA((total,)),
            pltpu.SemaphoreType.DMA((9,)),
            pltpu.SemaphoreType.DMA((2 * (n - 1) * total,)),
            pltpu.SemaphoreType.DMA((2 * (n - 1) * total,)),
            pltpu.SemaphoreType.REGULAR,
            pltpu.VMEM(train.shape, jnp.float32),
            pltpu.VMEM(step.shape, jnp.float32),
            pltpu.SemaphoreType.DMA((2,)),
            pltpu.SemaphoreType.DMA((2 * (n - 1),)),
            pltpu.SemaphoreType.DMA((2 * (n - 1),)),
        ],
        compiler_params=pltpu.CompilerParams(
            collective_id=0, has_side_effects=True, vmem_limit_bytes=47 * 2**20
        ),
        name="gather",
    )(*weights, *lows, *highs, train, step)


def flush_kernel(n, count, *refs):
    sources, held = refs[:count], refs[count]
    results, result = refs[count + 1 : 2 * count + 1], refs[2 * count + 1]
    token, sems, held_sems = refs[2 * count + 2 :]
    me = lax.axis_index("shard")
    depth = held.shape[1] // n
    pieces = last_pieces(held.shape[0])
    outer = (me == 0) | (me == n - 1)

    def each(act):
        for i, (source, to) in enumerate(zip(sources, results)):
            act(pltpu.make_async_copy(source, to, sems.at[i]))
        for i, (start, size) in enumerate(pieces):
            rows = pl.ds(start, size)
            late = outer & is_late(i, len(pieces))

            @pl.when(jnp.logical_not(late))
            def _():
                act(pltpu.make_async_copy(
                    held.at[rows, :], result.at[rows, :], held_sems.at[i]
                ))

            @pl.when(late)
            def _():
                here = (rows, pl.ds(pl.multiple_of(me * depth, 128), depth))
                act(pltpu.make_async_copy(held.at[here], result.at[here], held_sems.at[i]))

    each(lambda copy: copy.start())
    token[...] = jnp.zeros_like(token)
    each(lambda copy: copy.wait())


def flushed(n, done, held):
    vmem, hbm = pl.BlockSpec(memory_space=pltpu.VMEM), pl.BlockSpec(memory_space=pltpu.HBM)
    return pl.pallas_call(
        functools.partial(flush_kernel, n, len(done)),
        out_shape=[jax.ShapeDtypeStruct(x.shape, x.dtype) for x in (*done, held)]
        + [pltpu.VMEM((8, 128), jnp.float32)],
        in_specs=[vmem] * (len(done) + 1),
        out_specs=[hbm] * (len(done) + 1) + [vmem],
        scratch_shapes=[
            pltpu.SemaphoreType.DMA((len(done),)),
            pltpu.SemaphoreType.DMA((len(last_pieces(held.shape[0])),)),
        ],
        compiler_params=pltpu.CompilerParams(vmem_limit_bytes=2**20),
        name="flush",
    )(*done, held)


def lay_out(parts, flat):
    tp, n, _, part = parts.shape
    for row in range(flat.shape[0]):
        cells, at = [], row * 128
        while at < (row + 1) * 128:
            slot, lo = divmod(at, part)
            size = min(part - lo, (row + 1) * 128 - at)
            cells.append(parts[slot % tp, slot // tp, 0:1, lo : lo + size])
            at += size
        flat[row : row + 1, :] = jnp.concatenate(cells, axis=1) if len(cells) > 1 else cells[0]


def tail_kernel(n, tp, depth, held, line, token, tail, norm_out, *scratch):
    lines, norm_flat, send_sem, recv_sem, side_send, side_recv = scratch
    me, my_tp = lax.axis_index("shard"), lax.axis_index("tp")
    pieces = last_pieces(held.shape[0])
    ends = ((1, n - 1), (-1, 0))

    core = lax.rem(lax.axis_index("trial"), 2)
    pl.when((core == 1) & ((me == 0) | (me == n - 1)))(lambda: pl.delay(YIELD_NS))

    barrier = pltpu.get_barrier_semaphore()
    for way, at in ends:
        @pl.when(me == at)
        def _():
            pl.semaphore_signal(
                barrier, inc=1, device_id={"shard": at - way}, device_id_type=MESH
            )
    for t in range(1, tp):
        pl.semaphore_signal(
            barrier, inc=1, device_id={"tp": lax.rem(my_tp + t, tp)}, device_id_type=MESH
        )
    lines[my_tp] = line[...]
    greeted = sum(jnp.where(me == at - way, 1, 0) for way, at in ends) + tp - 1
    pl.when(greeted > 0)(lambda: pl.semaphore_wait(barrier, greeted))

    def each(way, at, away, act):
        for i, (start, size) in enumerate(pieces):
            here = (pl.ds(start, size), pl.ds(0 if way > 0 else depth, (n - 1) * depth))
            slot = (0 if way > 0 else len(pieces)) + i

            @pl.when((me == at - away) & is_late(i, len(pieces)))
            def _():
                act(pltpu.make_async_remote_copy(
                    held.at[here], tail.at[here], send_sem.at[slot], recv_sem.at[slot],
                    device_id={"shard": at}, device_id_type=MESH,
                ))

    def side(t, column):
        return pltpu.make_async_remote_copy(
            line, lines.at[column], side_send.at[t - 1], side_recv.at[t - 1],
            device_id={"tp": lax.rem(my_tp + t, tp)}, device_id_type=MESH,
        )

    for way, at in ends:
        each(way, at, way, lambda copy: copy.start())
    for t in range(1, tp):
        side(t, my_tp).start()
    for t in range(1, tp):
        side(t, lax.rem(my_tp - t + tp, tp)).wait_recv()
    lay_out(lines, norm_flat)
    norm_out[...] = norm_flat[...].astype(jnp.bfloat16)
    for way, at in ends:
        each(way, at, 0, lambda copy: copy.wait_recv())
    for way, at in ends:
        each(way, at, way, lambda copy: copy.wait_send())
    for t in range(1, tp):
        side(t, my_tp).wait_send()


def tailed(n, tp, depth, held, line, token):
    vmem = pl.BlockSpec(memory_space=pltpu.VMEM)
    count = len(last_pieces(held.shape[0]))
    lines = (tp, *line.shape)
    flat = (math.prod(lines) // 128, 128)
    return pl.pallas_call(
        functools.partial(tail_kernel, n, tp, depth),
        out_shape=[pltpu.VMEM(held.shape, held.dtype), pltpu.VMEM(flat, jnp.bfloat16)],
        in_specs=[vmem] * 3,
        out_specs=[vmem] * 2,
        scratch_shapes=[
            pltpu.VMEM(lines, jnp.float32),
            pltpu.VMEM(flat, jnp.float32),
            pltpu.SemaphoreType.DMA((2 * count,)),
            pltpu.SemaphoreType.DMA((2 * count,)),
            pltpu.SemaphoreType.DMA((max(tp - 1, 1),)),
            pltpu.SemaphoreType.DMA((max(tp - 1, 1),)),
        ],
        compiler_params=pltpu.CompilerParams(
            collective_id=1, has_side_effects=True, vmem_limit_bytes=2**20
        ),
        name="tail",
    )(held, line, token)


def close_kernel(n, tail, norm, begun, result, norm_out, sems):
    me = lax.axis_index("shard")
    pieces = last_pieces(tail.shape[0])
    depth = tail.shape[1] // n

    def each(act):
        for at in (0, n - 1):
            for i, (start, size) in enumerate(pieces):
                here = (pl.ds(start, size), pl.ds(0 if at else depth, (n - 1) * depth))

                @pl.when((me == at) & is_late(i, len(pieces)))
                def _():
                    act(pltpu.make_async_copy(tail.at[here], result.at[here], sems.at[i]))
        act(pltpu.make_async_copy(norm, norm_out, sems.at[len(pieces)]))

    each(lambda copy: copy.start())
    each(lambda copy: copy.wait())


def closed(n, tail, norm, begun):
    vmem, hbm = pl.BlockSpec(memory_space=pltpu.VMEM), pl.BlockSpec(memory_space=pltpu.HBM)
    return pl.pallas_call(
        functools.partial(close_kernel, n),
        out_shape=[jax.ShapeDtypeStruct(x.shape, x.dtype) for x in (begun, norm)],
        in_specs=[vmem, vmem, hbm],
        out_specs=[hbm] * 2,
        input_output_aliases={2: 0},
        scratch_shapes=[pltpu.SemaphoreType.DMA((len(last_pieces(tail.shape[0])) + 1,))],
        compiler_params=pltpu.CompilerParams(vmem_limit_bytes=2**20),
        name="close",
    )(tail, norm, begun)


def plain(weights, lows, highs, norm_new):
    serve = []
    for weight, low, high in zip(weights, lows, highs):
        fresh = weight.astype(jnp.float32) + mix_rate * jnp.dot(
            low, high, preferred_element_type=jnp.float32
        )
        serve.append(
            lax.all_gather(fresh.astype(jnp.bfloat16), "shard", axis=0, tiled=True).T
        )
    norm = lax.all_gather(
        norm_new.astype(jnp.bfloat16), ("shard", "tp"), axis=0, tiled=True
    )
    return (*serve, norm)


def on_device(n, tp, wq, lq, hq, wk, lk, hk, wv, lv, hv, norm_train, norm_step):
    weights, lows, highs = (wq, wk, wv), (lq, lk, lv), (hq, hk, hv)
    depth = wq.shape[0]
    if n < 2 or depth % 128 or any(w.shape[1] % ROWS or w.shape[1] < 2 * ROWS for w in weights):
        return plain(weights, lows, highs, norm_train + norm_step)
    query, key, value, line = gathered(
        n, ROWS, weights, [low.T for low in lows], highs, norm_train, norm_step
    )
    query, key, begun, token = flushed(n, [query, key], value)
    tail, norm = tailed(n, tp, depth, value, line, token)
    value, norm = closed(n, tail, norm, begun)
    return (query, key, value, norm.reshape(-1))


def solution(mesh):
    in_specs = (
        (P(("trial", "shard"), "tp"), P(("trial", "shard"), None), P("trial", "tp")) * 3
        + (P(("trial", "shard", "tp")),) * 2
    )
    out_specs = (P(("trial", "tp"), None),) * 3 + (P("trial"),)
    body = functools.partial(on_device, mesh.shape["shard"], mesh.shape["tp"])
    return jax.shard_map(
        body, mesh=mesh, in_specs=in_specs, out_specs=out_specs, check_vma=False
    )
```
